256 devices in a mesh: dp: 4 (over x), expert: 64 (over y, z, core).
Axes of the slice: x: 4, y: 4, z: 8, core: 2. Of those that a mesh axis runs over, the one named last changes fastest.
Arguments:
- hidden: bfloat16 [4, 4096, 2, 2048], P('dp', 'expert'), may hold values from -6 to 6
- queries: bfloat16 [4, 4096, 2, 4096], P('dp', 'expert'), may hold values from -45 to 45
- latents: bfloat16 [4, 4096, 2, 512], P('dp', 'expert'), may hold values from -165 to 165
- mem_latents: bfloat16 [4, 32, 2, 512], P('dp'), may hold values from -6 to 6
- lengths: int32 [4, 2], P('dp'), may hold values from 2048 to 4096
- ids: int32 [4, 4096, 2, 6], P('dp', 'expert'), may hold values from 0 to 63, all different within a row; in each aligned block of 128 rows (0 to 127, 128 to 255, ..., all dimensions but the last counted through in order) at most 14 rows name the same one
- gates: bfloat16 [4, 4096, 2, 6], P('dp', 'expert'), may hold values from 0.049804688 to 0.5
- norm_gain: bfloat16 [2048], replicated, may hold values from 0.25 to 1.75
- w_uv: bfloat16 [8, 512, 128], P('dp'), may hold values from -0.25 to 0.25
- w_out: bfloat16 [1024, 2048], P('dp'), may hold values from -0.1875 to 0.1875
- w_gate: bfloat16 [64, 2048, 704], P('expert'), may hold values from -0.125 to 0.125
- w_up: bfloat16 [64, 2048, 704], P('expert'), may hold values from -0.125 to 0.125
- w_down: bfloat16 [64, 704, 2048], P('expert'), may hold values from -0.21875 to 0.21875
Outputs:
- layer_out: bfloat16 [4, 4096, 2, 2048], P('dp', 'expert')
The draws below stay inside these ranges and needn't reach their ends.
Inputs may be any that keep to these rules, and one draw needn't show every extreme that they name: `ids`: each row names 6 different experts; the rows of one device (aligned blocks of 128 rows in the order of the leading dimensions) name any one expert at most 14 times, a bound that some block reaches.
All inputs are finite; a program needn't handle non-finite values.
Results may differ from the reference program's by a relative error of at most 0.007.
Values may be sent and summed in bfloat16 or wider, within the bound.
A program may use at most 128 MiB of HBM per device.

```python
import math
import jax
import jax.numpy as jnp
import numpy as np
from jax import lax

D = 2048
HEADS = 8
LAT = 512
VDIM = 128
FF = 704
TOPK = 6
MEM = 32
SEQS = 2
SEG = 4096
TOK_DEV = 128
EXPERTS = 64
CAP = 14
N_DP = 4
N_EXPERT = 64


def draw_latents(key, part):
    entries = jnp.clip(jax.random.normal(jax.random.fold_in(key, 1), (N_DP, SEG, SEQS, LAT), jnp.float32), -6.0, 6.0)
    return entries.astype(jnp.bfloat16)


def draw_queries(key, part):
    full_shape = (N_DP, SEG, SEQS, HEADS, LAT)
    entries = 0.5 * jnp.clip(jax.random.normal(jax.random.fold_in(key, 3), full_shape, jnp.float32), -6.0, 6.0)
    return entries.reshape(N_DP, SEG, SEQS, HEADS * LAT).astype(jnp.bfloat16)


def set_ends(drawn, rng, low, largest):
    spot = [jax.random.randint(jax.random.fold_in(rng, axis), (), 0, length) for axis, length in enumerate(drawn.shape)]
    longest = drawn.shape.index(max(drawn.shape))
    neighbour = spot[:longest] + [(spot[longest] + 1) % drawn.shape[longest]] + spot[longest + 1:]
    return drawn.at[tuple(spot)].set(low).at[tuple(neighbour)].set(largest)


def steps_of(key, extent, shards, least, high):
    level, own = 1.0, jax.random.fold_in(key, 6)
    for dim, parts in shards:
        heights = jnp.exp(jax.random.uniform(jax.random.fold_in(own, dim), (parts,), jnp.float32, least / len(shards), high / len(shards)))
        level = level * jnp.repeat(heights, extent[dim] // parts).reshape([-1 if axis == dim else 1 for axis in range(len(extent))])
    return level


def routed_block(own_key, own, number, rows, number_of, top, most, slope):
    ranking = jax.random.permutation(own_key, number_of)
    crowded, ordinary = portions_of(number_of, rows * top, most, slope, True), portions_of(number_of, rows * top, most, slope, False)
    places = jnp.arange(number_of)

    def named(sizes, offset_by):
        used = int((sizes > 0).sum())
        fixed = max(1, used // 4)
        moved = fixed + (places - fixed + offset_by * (used - fixed)) % max(1, number_of - fixed)
        return jnp.zeros((number_of,), jnp.int32).at[ranking[jnp.where(places < fixed, places, moved)]].set(jnp.asarray(sizes, jnp.int32))

    sizes = jnp.where(number % 4 == 0, named(crowded, number // 4), named(ordinary, number - number // 4 - 1))
    mixed = jax.random.permutation(jax.random.fold_in(own, 3), number_of)
    giver, sink = mixed[0:number_of // 2 * 2:2], mixed[1:number_of // 2 * 2:2]
    margin = jnp.minimum(sizes[giver] - 1, most - sizes[sink]) // 2
    margin = jnp.where((giver == ranking[0]) | (sink == ranking[0]) | (sizes[sink] == 0), 0, jnp.maximum(margin, 0))
    moved = jax.random.randint(jax.random.fold_in(own, 4), (number_of // 2,), 0, 1 << 20) % (margin + 1)
    sizes = sizes.at[giver].add(-moved).at[sink].add(moved)
    labels = jnp.searchsorted(jnp.cumsum(sizes), jnp.arange(rows * top), side="right").astype(jnp.int32)
    table = labels.reshape(top, rows).T
    table = table[jax.random.permutation(jax.random.fold_in(own, 1), rows)]
    offset_by = jax.random.randint(jax.random.fold_in(own, 2), (rows, 1), 0, top)
    return jnp.take_along_axis(table, (jnp.arange(top)[None, :] + offset_by) % top, axis=1)


def portions_of(number_of, total, reach, skew, full):
    weights = [(1 << 20) // math.isqrt(grade ** skew) + 1 for grade in range(1, number_of + 1)]
    largest = reach if full else min(reach, max(-(-total // number_of), total * weights[0] // sum(weights)))
    least = 1 if total - largest >= number_of - 1 else 0
    given, surplus = [largest] + [least] * (number_of - 1), total - largest - least * (number_of - 1)
    while surplus > 0:
        candidates = [i for i in range(1, number_of) if given[i] < largest] or [i for i in range(1, number_of) if given[i] < reach]
        pool, budget = sum([weights[i] for i in candidates]), surplus
        for i in candidates:
            extra = min(reach - given[i], max(1, budget * weights[i] // pool), surplus)
            given[i] = given[i] + extra
            surplus = surplus - extra
    return np.array(given)


def scatter_about(key, shape, scale, most, cuts=(), held_as=jnp.bfloat16):
    values = jax.random.normal(key, shape, jnp.float32) * scale
    if len(cuts) > 0:
        values = steps_of(key, shape, cuts, -0.22, 0.18) * values
    return jnp.clip(values, min=-most, max=most).astype(held_as)


def setup_inputs(seed: int = 0) -> dict:
    arg_keys = jax.random.split(jax.random.key(seed), 14)
    hidden = scatter_about(arg_keys[0], (N_DP, SEG, SEQS, D), 1.0, 6.0, ((0, 4), (1, 64)))
    queries = draw_queries(jax.random.fold_in(arg_keys[13], 71), 0)
    latents = draw_latents(jax.random.fold_in(arg_keys[13], 71), 0)
    mem_latents = scatter_about(arg_keys[3], (N_DP, MEM, SEQS, LAT), 1.0, 6.0, ((0, 4),))
    lengths = set_ends(jax.random.randint(arg_keys[4], (N_DP, SEQS), SEG // 2, SEG + 1), jax.random.fold_in(arg_keys[4], 1), SEG // 2, SEG).astype(jnp.int32)
    ids_keys = jax.random.split(jax.random.fold_in(arg_keys[5], 1), N_DP * SEG * SEQS // TOK_DEV)
    ids_turns = jax.random.permutation(jax.random.fold_in(arg_keys[5], 3), N_DP * SEG * SEQS // TOK_DEV)
    ids = jax.vmap(lambda own, number: routed_block(jax.random.fold_in(arg_keys[5], 2), own, number, TOK_DEV, EXPERTS, TOPK, CAP, 2))(ids_keys, ids_turns).reshape((N_DP, SEG, SEQS, TOPK))
    gates = jnp.clip(jnp.exp(math.log(0.5) - 2.306499 * jax.random.uniform(arg_keys[6], (N_DP, SEG, SEQS, TOPK), jnp.float32) ** steps_of(arg_keys[6], (N_DP, SEG, SEQS, TOPK), ((0, 4), (1, 64)), -0.2, 0.2)), 0.049804688, 0.5).astype(jnp.bfloat16)
    norm_gain = jnp.clip(1.0 + 0.15 * jax.random.normal(arg_keys[7], (D,), jnp.float32), 0.25, 1.75).astype(jnp.bfloat16)
    w_uv = scatter_about(arg_keys[8], (HEADS, LAT, VDIM), LAT ** -0.5, 0.25, ((0, 4),))
    w_out = scatter_about(arg_keys[9], (HEADS * VDIM, D), (HEADS * VDIM) ** -0.5, 0.1875, ((0, 4),))
    w_gate = scatter_about(arg_keys[10], (EXPERTS, D, FF), D ** -0.5, 0.125, ((0, 64),))
    w_up = scatter_about(arg_keys[11], (EXPERTS, D, FF), D ** -0.5, 0.125, ((0, 64),))
    w_down = scatter_about(arg_keys[12], (EXPERTS, FF, D), FF ** -0.5, 0.21875, ((0, 64),))
    return {"hidden": hidden, "queries": queries, "latents": latents, "mem_latents": mem_latents, "lengths": lengths, "ids": ids, "gates": gates, "norm_gain": norm_gain, "w_uv": w_uv, "w_out": w_out, "w_gate": w_gate, "w_up": w_up, "w_down": w_down}


score_scale = 192.0 ** (-0.5)
norm_eps = 1e-06

def attend_one(query_rows, seg_latent, mem_latent, seq_limit):
    key_rows = jnp.concatenate([mem_latent, seg_latent], axis=0).astype(jnp.float32)
    scores = jnp.einsum('ihl,jl->hij', query_rows.astype(jnp.float32), key_rows) * score_scale
    query_pos = jnp.arange(SEG, dtype=jnp.int32)
    seg_visible = (query_pos[None, :] <= query_pos[:, None]) & (query_pos[None, :] < seq_limit)
    visible = jnp.concatenate([jnp.ones((SEG, MEM), dtype=bool), seg_visible], axis=1)
    scores = jnp.where(visible[None], scores, -jnp.inf)
    row_top = lax.optimization_barrier(jnp.max(scores, axis=2))
    weights = jnp.exp(scores - row_top[..., None])
    exp_total = lax.optimization_barrier(jnp.sum(weights, axis=2))
    rounded = lax.optimization_barrier(weights.astype(jnp.bfloat16)).astype(jnp.float32)
    attended = jnp.einsum('hij,jl->ihl', rounded, key_rows) / jnp.transpose(exp_total)[..., None]
    return attended.astype(jnp.bfloat16)

def reference(hidden, queries, latents, mem_latents, lengths, ids, gates, norm_gain, w_uv, w_out, w_gate, w_up, w_down):
    batch = N_DP * SEQS
    query_all = queries.reshape(N_DP, SEG, SEQS, HEADS, LAT).transpose(0, 2, 1, 3, 4).reshape(batch, SEG, HEADS, LAT)
    seg_all = latents.transpose(0, 2, 1, 3).reshape(batch, SEG, LAT)
    mem_all = mem_latents.transpose(0, 2, 1, 3).reshape(batch, MEM, LAT)
    limits = lengths.reshape(batch)
    attended = lax.map(lambda item: attend_one(item[0], item[1], item[2], item[3]), (query_all, seg_all, mem_all, limits))
    values = jnp.einsum('bihl,hlv->bihv', attended.astype(jnp.float32), w_uv.astype(jnp.float32)).astype(jnp.bfloat16)
    attn_out = jnp.dot(values.reshape(batch * SEG, HEADS * VDIM), w_out, preferred_element_type=jnp.float32)
    attn_out = attn_out.reshape(N_DP, SEQS, SEG, D).transpose(0, 2, 1, 3)
    residual = hidden.astype(jnp.float32) + attn_out
    mean_square = lax.optimization_barrier(jnp.mean(residual * residual, axis=-1, keepdims=True))
    normed = (residual * lax.rsqrt(mean_square + norm_eps) * norm_gain.astype(jnp.float32)).astype(jnp.bfloat16)
    row_total = N_DP * SEG * SEQS
    flat_normed = normed.reshape(row_total, D)
    flat_ids = ids.reshape(row_total * TOPK)
    flat_gates = gates.reshape(row_total * TOPK).astype(jnp.float32)
    reach_rows = N_DP * N_EXPERT * CAP

    def per_expert(running, item):
        gate_w, up_w, down_w, expert_id = item
        matches = flat_ids == expert_id
        picked = jnp.nonzero(matches, size=reach_rows, fill_value=0)[0].astype(jnp.int32)
        is_live = jnp.arange(reach_rows, dtype=jnp.int32) < jnp.sum(matches.astype(jnp.int32))
        token_index = (picked // TOPK).astype(jnp.int32)
        picked_rows = flat_normed[token_index]
        gate_h = jnp.dot(picked_rows, gate_w, preferred_element_type=jnp.float32)
        up_h = jnp.dot(picked_rows, up_w, preferred_element_type=jnp.float32)
        act = (jax.nn.silu(gate_h) * up_h).astype(jnp.bfloat16)
        out_rows = jnp.dot(act, down_w, preferred_element_type=jnp.float32).astype(jnp.bfloat16)
        out_rows = lax.optimization_barrier(out_rows).astype(jnp.float32)
        scale_w = jnp.where(is_live, flat_gates[picked], jnp.float32(0.0))
        running = running.at[token_index].add(scale_w[:, None] * out_rows)
        return (running, None)
    start_acc = jnp.zeros((row_total, D), jnp.float32)
    routed, unused = lax.scan(per_expert, start_acc, (w_gate, w_up, w_down, jnp.arange(EXPERTS, dtype=jnp.int32)))
    layer_out = residual + routed.reshape(N_DP, SEG, SEQS, D)
    return layer_out.astype(jnp.bfloat16)
```

```python
import jax
import jax.numpy as jnp
from jax import lax
from jax.experimental import pallas as pl
from jax.experimental.pallas import tpu as pltpu
from jax.sharding import PartitionSpec as P

score_scale = 192.0 ** (-0.5)
norm_eps = 1e-06
NY, NZ, NC = 4, 8, 2
Q = 8
TOK = 128
CAP = 14
EXPERTS = 64
PEERS = NY * NC
ROWS = NZ * CAP
ALLROWS = PEERS * ROWS


def place():
    me = lax.axis_index("expert")
    c = lax.rem(me, NC)
    z = lax.rem(lax.div(me, NC), NZ)
    y = lax.div(me, NC * NZ)
    return me, y, z, c


def device_at(y, z, c):
    return (y * NZ + z) * NC + c


def wrap(v, n):
    return lax.rem(v + 2 * n, n)


def send(src, dst, ssem, rsem, to):
    return pltpu.make_async_remote_copy(
        src_ref=src,
        dst_ref=dst,
        send_sem=ssem,
        recv_sem=rsem,
        device_id={"expert": to},
        device_id_type=pl.DeviceIdType.MESH,
    )


def bdot(a, b):
    return jnp.dot(a, b, preferred_element_type=jnp.float32)


def expert_kernel(
    nq_hbm, resid_hbm, ids_ref, gates_ref, wg_hbm, wu_hbm, wd_hbm, out_ref,
    xs, place_m, mix_m, sent, got, gate_acc, up_acc, act, wg, wu, wd, back, part, landed, resid, table,
    load_sem, zsend, zrecv, ysend, yrecv, osend, orecv, rsend, rrecv, tsend, trecv,
):
    width = xs.shape[3]
    me, y, z, c = place()
    my_slot = y * NC + c

    loads = [
        pltpu.make_async_copy(nq_hbm, xs.at[z], load_sem.at[0]),
        pltpu.make_async_copy(wg_hbm, wg, load_sem.at[1]),
        pltpu.make_async_copy(wu_hbm, wu, load_sem.at[2]),
        pltpu.make_async_copy(wd_hbm, wd, load_sem.at[3]),
        pltpu.make_async_copy(resid_hbm, resid, load_sem.at[4]),
    ]
    for load in loads:
        load.start()

    barrier = pltpu.get_barrier_semaphore()
    partners = []
    for k in range(1, PEERS):
        slot = wrap(my_slot + k, PEERS)
        partners.append(device_at(lax.div(slot, NC), z, lax.rem(slot, NC)))
    around = [device_at(y, wrap(z + 1, NZ), c), device_at(y, wrap(z - 1, NZ), c)]
    for dev in partners + around:
        pl.semaphore_signal(barrier, inc=1, device_id={"expert": dev}, device_id_type=pl.DeviceIdType.MESH)

    expert_iota = lax.broadcasted_iota(jnp.int32, (EXPERTS, TOK), 0)
    hits = []
    named = jnp.zeros((EXPERTS, TOK), jnp.float32)
    for k in range(6):
        hit = expert_iota == jnp.broadcast_to(ids_ref[k : k + 1, :], (EXPERTS, TOK))
        hits.append(hit)
        named = named + jnp.where(hit, 1.0, 0.0)
    earlier = lax.broadcasted_iota(jnp.int32, (TOK, TOK), 0) < lax.broadcasted_iota(jnp.int32, (TOK, TOK), 1)
    before = bdot(named.astype(jnp.bfloat16), jnp.where(earlier, 1.0, 0.0).astype(jnp.bfloat16))
    expert_base = (expert_iota * CAP + z * (EXPERTS * CAP)).astype(jnp.float32)
    rows = []
    for k in range(6):
        rows.append(jnp.sum(jnp.where(hits[k], before + expert_base, 0.0), axis=0, keepdims=True))
    filler = jnp.full((2, TOK), -1.0, jnp.float32)
    table[z] = jnp.concatenate(rows + [filler, gates_ref[...]], axis=0)

    pl.semaphore_wait(barrier, len(partners) + len(around))
    loads[0].wait()

    def z_copy(block, j, sem_slot, to):
        return send(xs.at[block, j], xs.at[block, j], zsend.at[j, sem_slot], zrecv.at[j, block], to)

    def t_copy(block, sem_slot, to):
        return send(table.at[block], table.at[block], tsend.at[sem_slot], trecv.at[block], to)

    def y_copy(k, j):
        slot = wrap(my_slot + k, PEERS)
        to = device_at(lax.div(slot, NC), z, lax.rem(slot, NC))
        return send(sent.at[j, slot], got.at[j, my_slot], ysend.at[j, k], yrecv.at[j, my_slot], to)

    def wait_y(k, j):
        slot = wrap(my_slot + k, PEERS)
        to = device_at(lax.div(slot, NC), z, lax.rem(slot, NC))
        send(sent.at[j, slot], got.at[j, slot], ysend.at[j, k], yrecv.at[j, slot], to).wait_recv()

    def o_copy(k, j):
        slot = wrap(my_slot + k, PEERS)
        to = device_at(lax.div(slot, NC), z, lax.rem(slot, NC))
        return send(sent.at[j, slot], back.at[j, my_slot], osend.at[j, k], orecv.at[j, my_slot], to)

    def wait_o(k, j):
        slot = wrap(my_slot + k, PEERS)
        to = device_at(lax.div(slot, NC), z, lax.rem(slot, NC))
        send(sent.at[j, slot], back.at[j, slot], osend.at[j, k], orecv.at[j, slot], to).wait_recv()

    def direction(j):
        return 1 - 2 * lax.rem(j, 2)

    def z_major(j, s):
        d = direction(j)
        return z_copy(wrap(z - d * s, NZ), j, s, device_at(y, wrap(z + d, NZ), c))

    def z_minor(j, s):
        d = direction(j)
        return z_copy(wrap(z + d * s, NZ), j, 4 + s, device_at(y, wrap(z - d, NZ), c))

    def t_major(s):
        return t_copy(wrap(z - s, NZ), s, device_at(y, wrap(z + 1, NZ), c))

    def t_minor(s):
        return t_copy(wrap(z + s, NZ), 4 + s, device_at(y, wrap(z - 1, NZ), c))

    def build_tables():
        r = lax.broadcasted_iota(jnp.int32, (ALLROWS, TOK), 0)
        group = lax.shift_right_logical(r * 9363, 17)
        within = r - group * CAP
        peer = lax.shift_right_logical(group, 3)
        block = group - peer * NZ
        owner_y = lax.shift_right_logical(peer, 1)
        owner_c = peer - owner_y * NC
        owner = (owner_y * NZ + z) * NC + owner_c
        code = (block * (EXPERTS * CAP) + owner * CAP + within).astype(jnp.float32)

        def one_block(b, carry):
            rows_b = table[b]
            hot = jnp.zeros((ALLROWS, TOK), jnp.float32)
            mixed = jnp.zeros((ALLROWS, TOK), jnp.float32)
            for k in range(6):
                hit = code == jnp.broadcast_to(rows_b[k : k + 1, :], (ALLROWS, TOK))
                hot = jnp.where(hit, 1.0, hot)
                mixed = jnp.where(hit, jnp.broadcast_to(rows_b[8 + k : 9 + k, :], (ALLROWS, TOK)), mixed)
            place_m[:, pl.ds(pl.multiple_of(b * TOK, TOK), TOK)] = hot.astype(jnp.bfloat16)
            mix_m[b] = mixed.T.astype(jnp.bfloat16)
            return carry

        lax.fori_loop(0, NZ, one_block, 0)

    gate_acc[...] = jnp.zeros_like(gate_acc)
    up_acc[...] = jnp.zeros_like(up_acc)

    def dispatch_step(i, carry):
        for s in range(4):
            j = i - s

            @pl.when((j >= 0) & (j < Q))
            def _():
                d = direction(j)
                block = wrap(z - d * s, NZ)
                copy = z_major(j, s)
                if s > 0:
                    z_copy(block, j, s, device_at(y, wrap(z + d, NZ), c)).wait_recv()
                copy.start()
                if s < 3:
                    block2 = wrap(z + d * s, NZ)
                    copy2 = z_minor(j, s)
                    if s > 0:
                        z_copy(block2, j, 4 + s, device_at(y, wrap(z - d, NZ), c)).wait_recv()
                    copy2.start()

        for s in range(4):

            @pl.when(i == s)
            def _():
                copy = t_major(s)
                if s > 0:
                    copy.wait_recv()
                copy.start()
                if s < 3:
                    copy2 = t_minor(s)
                    if s > 0:
                        copy2.wait_recv()
                    copy2.start()

        @pl.when(i == 4)
        def _():
            t_copy(wrap(z - 4, NZ), 0, me).wait_recv()
            t_copy(wrap(z + 3, NZ), 0, me).wait_recv()
            build_tables()

        j = i - 4

        @pl.when((j >= 0) & (j < Q))
        def _():
            d = direction(j)
            z_copy(wrap(z - 4 * d, NZ), j, 0, me).wait_recv()
            z_copy(wrap(z + 3 * d, NZ), j, 0, me).wait_recv()
            block_rows = xs[:, j].reshape(NZ * TOK, width)
            packed = bdot(place_m[...], block_rows).astype(jnp.bfloat16)
            sent[j] = packed.reshape(PEERS, ROWS, width)
            got[j, my_slot] = sent[j, my_slot]

        j2 = i - 6

        @pl.when(j2 >= 0)
        def _():
            @pl.when(j2 == 0)
            def _():
                loads[1].wait()
                loads[2].wait()

            for k in range(1, PEERS):
                wait_y(k, j2)
            x = got[j2].reshape(ALLROWS, width)
            cols = pl.ds(pl.multiple_of(j2 * width, width), width)
            gate_acc[...] += bdot(x, wg[cols, :])
            up_acc[...] += bdot(x, wu[cols, :])

        @pl.when((j >= 0) & (j < Q))
        def _():
            for k in range(1, PEERS):
                y_copy(k, j).start()

        return carry

    lax.fori_loop(0, Q + 6, dispatch_step, 0)

    g = gate_acc[...]
    act[...] = ((g / (1.0 + jnp.exp(-g))) * up_acc[...]).astype(jnp.bfloat16)
    loads[3].wait()
    loads[4].wait()

    def drain_dispatch(j, carry):
        for s in range(4):
            z_major(j, s).wait_send()
            if s < 3:
                z_minor(j, s).wait_send()
        for k in range(1, PEERS):
            y_copy(k, j).wait_send()
        return carry

    lax.fori_loop(0, Q, drain_dispatch, 0)
    for s in range(4):
        t_major(s).wait_send()
        if s < 3:
            t_minor(s).wait_send()

    def r_major(j, s):
        return send(xs.at[s, j], landed.at[s, j], rsend.at[j, s], rrecv.at[j, s],
                    device_at(y, wrap(z + direction(j), NZ), c))

    def r_minor(j, s):
        return send(xs.at[4 + s, j], landed.at[4 + s, j], rsend.at[j, 4 + s], rrecv.at[j, 4 + s],
                    device_at(y, wrap(z - direction(j), NZ), c))

    def combine_step(i, carry):
        @pl.when(i < Q)
        def _():
            cols = pl.ds(pl.multiple_of(i * width, width), width)
            made = bdot(act[...], wd[:, cols]).astype(jnp.bfloat16)
            sent[i] = made.reshape(PEERS, ROWS, width)
            back[i, my_slot] = sent[i, my_slot]

        jm = i - 2

        @pl.when((jm >= 0) & (jm < Q))
        def _():
            for k in range(1, PEERS):
                wait_o(k, jm)
            rows_in = back[jm].reshape(ALLROWS, width)
            mixed = bdot(mix_m[...].reshape(NZ * TOK, ALLROWS), rows_in)
            part[jm] = mixed.reshape(NZ, TOK, width)

        for s in (3, 2, 1, 0):
            j = i - 2 - s

            @pl.when((j >= 0) & (j < Q))
            def _():
                d = direction(j)
                value = part[j, wrap(z + d * (4 - s), NZ)]
                if s > 0:
                    r_major(j, s - 1).wait_recv()
                    value = value + landed[s - 1, j].astype(jnp.float32)
                xs[s, j] = value.astype(jnp.bfloat16)
                if s < 3:
                    value2 = part[j, wrap(z - d * (3 - s), NZ)]
                    if s > 0:
                        r_minor(j, s - 1).wait_recv()
                        value2 = value2 + landed[4 + s - 1, j].astype(jnp.float32)
                    xs[4 + s, j] = value2.astype(jnp.bfloat16)

        for s in (3, 2, 1, 0):
            j = i - 2 - s

            @pl.when((j >= 0) & (j < Q))
            def _():
                r_major(j, s).start()
                if s < 3:
                    r_minor(j, s).start()

        @pl.when(i < Q)
        def _():
            for k in range(1, PEERS):
                o_copy(k, i).start()

        jf = i - 6

        @pl.when((jf >= 0) & (jf < Q))
        def _():
            r_major(jf, 3).wait_recv()
            r_minor(jf, 2).wait_recv()
            total = part[jf, z] + landed[3, jf].astype(jnp.float32) + landed[6, jf].astype(jnp.float32)
            cols = pl.ds(pl.multiple_of(jf * width, width), width)
            out_ref[:, cols] = (resid[:, cols] + total).astype(jnp.bfloat16)

        return carry

    lax.fori_loop(0, Q + 6, combine_step, 0)

    def drain_combine(j, carry):
        for s in range(4):
            r_major(j, s).wait_send()
            if s < 3:
                r_minor(j, s).wait_send()
        for k in range(1, PEERS):
            o_copy(k, j).wait_send()
        return carry

    lax.fori_loop(0, Q, drain_combine, 0)


def run_experts(nq, resid, ids_t, gates_t, w_gate, w_up, w_down):
    width = nq.shape[2]
    model_width = w_gate.shape[0]
    hidden_units = w_gate.shape[1]
    anywhere = pl.BlockSpec(memory_space=pl.ANY)
    vmem = pl.BlockSpec(memory_space=pltpu.VMEM)
    bf16, f32 = jnp.bfloat16, jnp.float32
    dma = pltpu.SemaphoreType.DMA
    return pl.pallas_call(
        expert_kernel,
        out_shape=jax.ShapeDtypeStruct((TOK, model_width), bf16),
        in_specs=[anywhere, anywhere, vmem, vmem, anywhere, anywhere, anywhere],
        out_specs=vmem,
        scratch_shapes=[
            pltpu.VMEM((NZ, Q, TOK, width), bf16),
            pltpu.VMEM((ALLROWS, NZ * TOK), bf16),
            pltpu.VMEM((NZ, TOK, ALLROWS), bf16),
            pltpu.VMEM((Q, PEERS, ROWS, width), bf16),
            pltpu.VMEM((Q, PEERS, ROWS, width), bf16),
            pltpu.VMEM((ALLROWS, hidden_units), f32),
            pltpu.VMEM((ALLROWS, hidden_units), f32),
            pltpu.VMEM((ALLROWS, hidden_units), bf16),
            pltpu.VMEM((model_width, hidden_units), bf16),
            pltpu.VMEM((model_width, hidden_units), bf16),
            pltpu.VMEM((hidden_units, model_width), bf16),
            pltpu.VMEM((Q, PEERS, ROWS, width), bf16),
            pltpu.VMEM((Q, NZ, TOK, width), f32),
            pltpu.VMEM((7, Q, TOK, width), bf16),
            pltpu.VMEM((TOK, model_width), f32),
            pltpu.VMEM((NZ, 16, TOK), f32),
            dma((5,)),
            dma((Q, 7)), dma((Q, NZ)), dma((Q, PEERS)), dma((Q, PEERS)), dma((Q, PEERS)), dma((Q, PEERS)),
            dma((Q, 7)), dma((Q, 7)), dma((7,)), dma((NZ,)),
        ],
        compiler_params=pltpu.CompilerParams(
            collective_id=1, has_side_effects=True, vmem_limit_bytes=60 * 1024 * 1024
        ),
        name="experts",
    )(nq, resid, ids_t, gates_t, w_gate, w_up, w_down)


def sent_to_all(shard, axis):
    devices = lax.axis_size(axis)
    return lax.all_to_all(
        jnp.broadcast_to(shard[None], (devices, *shard.shape)), axis, 0, 0, tiled=True
    )


def joined_along(blocks, dim):
    dims = list(blocks.shape[1:])
    dims[dim] *= blocks.shape[0]
    return jnp.moveaxis(blocks, 0, dim).reshape(dims)


def gather_directly(shard, axis, dim):
    blocks = sent_to_all(shard, axis)
    return joined_along(blocks, dim)


def shards(
    hidden,
    queries,
    latents,
    mem_latents,
    lengths,
    ids,
    gates,
    norm_gain,
    w_uv,
    w_out,
    w_gate,
    w_up,
    w_down,
):
    local_len = hidden.shape[1]
    seq_count = hidden.shape[2]
    model_width = hidden.shape[3]
    latent_dim = latents.shape[3]
    head_count = queries.shape[3] // latent_dim
    row_count = local_len * seq_count
    owner_count = lax.axis_size("expert")
    shard_index = lax.axis_index("expert")
    own_pos = shard_index * local_len + jnp.arange(local_len, dtype=jnp.int32)
    query_rows = queries[0].reshape(local_len, seq_count, head_count, latent_dim)
    memory = mem_latents[0]
    seq_limit = lengths[0]
    mem_scores = (
        jnp.einsum("tshl,msl->shtm", query_rows, memory, preferred_element_type=jnp.float32)
        * score_scale
    )
    first_max = jnp.max(mem_scores, axis=3)
    mem_weights = jnp.exp(mem_scores - first_max[..., None])
    first_sum = jnp.sum(mem_weights, axis=3)
    first_acc = jnp.einsum(
        "shtm,msl->tshl",
        mem_weights.astype(jnp.bfloat16),
        memory,
        preferred_element_type=jnp.float32,
    )

    def fold_step(carry, portion):
        old_max, old_sum, old_acc = carry
        key_rows = portion[0]
        key_pos = jnp.arange(key_rows.shape[0], dtype=jnp.int32)
        scores = (
            jnp.einsum("tshl,jsl->shtj", query_rows, key_rows, preferred_element_type=jnp.float32)
            * score_scale
        )
        causal = key_pos[None, :] <= own_pos[:, None]
        inside = key_pos[None, :] < seq_limit[:, None]
        visible = causal[None, None, :, :] & inside[:, None, None, :]
        scores = jnp.where(visible, scores, -jnp.inf)
        new_max = jnp.maximum(old_max, jnp.max(scores, axis=3))
        weights = jnp.exp(scores - new_max[..., None])
        factor = jnp.exp(old_max - new_max)
        new_sum = old_sum * factor + jnp.sum(weights, axis=3)
        contrib = jnp.einsum(
            "shtj,jsl->tshl",
            weights.astype(jnp.bfloat16),
            key_rows,
            preferred_element_type=jnp.float32,
        )
        new_acc = old_acc * jnp.transpose(factor, (2, 0, 1))[..., None] + contrib
        return (new_max, new_sum, new_acc)

    portion = lax.all_gather(latents, "expert", axis=1, tiled=True)
    last_pos = jnp.max(own_pos)
    final_max, final_sum, final_acc = lax.cond(
        jnp.int32(0) <= last_pos,
        lambda state: fold_step(state, portion),
        lambda state: state,
        (first_max, first_sum, first_acc),
    )
    attended = (final_acc / jnp.transpose(final_sum, (2, 0, 1))[..., None]).astype(jnp.bfloat16)
    values = jnp.einsum(
        "tshl,hlv->tshv",
        attended,
        gather_directly(w_uv, "dp", 0),
        preferred_element_type=jnp.float32,
    ).astype(jnp.bfloat16)
    flat_values = values.reshape(row_count, -1)
    attn_out = jnp.dot(
        flat_values,
        lax.all_gather(w_out, "dp", axis=0, tiled=True),
        preferred_element_type=jnp.float32,
    )
    residual = hidden[0].reshape(row_count, model_width).astype(jnp.float32) + attn_out
    mean_square = jnp.mean(residual * residual, axis=-1, keepdims=True)
    normed = (residual * lax.rsqrt(mean_square + norm_eps) * norm_gain.astype(jnp.float32)).astype(
        jnp.bfloat16
    )
    width = model_width // Q
    nq = jnp.moveaxis(normed.reshape(row_count, Q, width), 1, 0)
    ids_t = jnp.pad(ids[0].reshape(row_count, -1).T, ((0, 2), (0, 0)), constant_values=-1)
    gates_t = jnp.pad(gates[0].reshape(row_count, -1).T.astype(jnp.float32), ((0, 2), (0, 0)))
    layer_out = run_experts(nq, residual, ids_t, gates_t, w_gate[0], w_up[0], w_down[0])
    return layer_out.reshape(1, local_len, seq_count, model_width)


def solution(mesh):
    return jax.shard_map(
        shards,
        mesh=mesh,
        in_specs=(
            P("dp", "expert", None, None),
            P("dp", "expert", None, None),
            P("dp", "expert", None, None),
            P("dp", None, None, None),
            P("dp", None),
            P("dp", "expert", None, None),
            P("dp", "expert", None, None),
            P(),
            P("dp", None, None),
            P("dp", None),
            P("expert", None, None),
            P("expert", None, None),
            P("expert", None, None),
        ),
        out_specs=P("dp", "expert", None, None),
        check_vma=False,
    )
```

```python
import jax
import jax.numpy as jnp
from jax import lax
from jax.experimental import pallas as pl
from jax.experimental.pallas import tpu as pltpu
from jax.sharding import PartitionSpec as P

score_scale = 192.0 ** (-0.5)
norm_eps = 1e-06


NY, NZ, NC = 4, 8, 2
Q = 8
TOK = 128
CAP = 14
EXPERTS = 64
PEERS = NY * NC
ROWS = NZ * CAP
ALLROWS = PEERS * ROWS


def place():
    me = lax.axis_index("expert")
    c = lax.rem(me, NC)
    z = lax.rem(lax.div(me, NC), NZ)
    y = lax.div(me, NC * NZ)
    return me, y, z, c


def device_at(y, z, c):
    return (y * NZ + z) * NC + c


def wrap(v, n):
    return lax.rem(v + 2 * n, n)


def send(src, dst, ssem, rsem, to):
    return pltpu.make_async_remote_copy(
        src_ref=src,
        dst_ref=dst,
        send_sem=ssem,
        recv_sem=rsem,
        device_id={"expert": to},
        device_id_type=pl.DeviceIdType.MESH,
    )


def bdot(a, b):
    return jnp.dot(a, b, preferred_element_type=jnp.float32)


def expert_kernel(
    nq_hbm, resid_hbm, ids_ref, gates_ref, wg_hbm, wu_hbm, wd_hbm, out_ref,
    xs, place_m, mix_m, sent, got, gate_acc, up_acc, act, wg, wu, wd, back, part, landed, resid, table,
    load_sem, zsend, zrecv, ysend, yrecv, osend, orecv, rsend, rrecv, tsend, trecv,
):
    width = xs.shape[3]
    me, y, z, c = place()
    my_slot = y * NC + c

    loads = [
        pltpu.make_async_copy(nq_hbm, xs.at[z], load_sem.at[0]),
        pltpu.make_async_copy(wg_hbm, wg, load_sem.at[1]),
        pltpu.make_async_copy(wu_hbm, wu, load_sem.at[2]),
        pltpu.make_async_copy(wd_hbm, wd, load_sem.at[3]),
        pltpu.make_async_copy(resid_hbm, resid, load_sem.at[4]),
    ]
    for load in loads:
        load.start()

    barrier = pltpu.get_barrier_semaphore()
    partners = []
    for k in range(1, PEERS):
        slot = wrap(my_slot + k, PEERS)
        partners.append(device_at(lax.div(slot, NC), z, lax.rem(slot, NC)))
    around = [device_at(y, wrap(z + 1, NZ), c), device_at(y, wrap(z - 1, NZ), c)]
    for dev in partners + around:
        pl.semaphore_signal(barrier, inc=1, device_id={"expert": dev}, device_id_type=pl.DeviceIdType.MESH)

    expert_iota = lax.broadcasted_iota(jnp.int32, (EXPERTS, TOK), 0)
    hits = []
    named = jnp.zeros((EXPERTS, TOK), jnp.float32)
    for k in range(6):
        hit = expert_iota == jnp.broadcast_to(ids_ref[k : k + 1, :], (EXPERTS, TOK))
        hits.append(hit)
        named = named + jnp.where(hit, 1.0, 0.0)
    earlier = lax.broadcasted_iota(jnp.int32, (TOK, TOK), 0) < lax.broadcasted_iota(jnp.int32, (TOK, TOK), 1)
    before = bdot(named.astype(jnp.bfloat16), jnp.where(earlier, 1.0, 0.0).astype(jnp.bfloat16))
    expert_base = (expert_iota * CAP + z * (EXPERTS * CAP)).astype(jnp.float32)
    rows = []
    for k in range(6):
        rows.append(jnp.sum(jnp.where(hits[k], before + expert_base, 0.0), axis=0, keepdims=True))
    filler = jnp.full((2, TOK), -1.0, jnp.float32)
    table[z] = jnp.concatenate(rows + [filler, gates_ref[...]], axis=0)

    pl.semaphore_wait(barrier, len(partners) + len(around))
    loads[0].wait()

    def z_copy(block, j, sem_slot, to):
        return send(xs.at[block, j], xs.at[block, j], zsend.at[j, sem_slot], zrecv.at[j, block], to)

    def t_copy(block, sem_slot, to):
        return send(table.at[block], table.at[block], tsend.at[sem_slot], trecv.at[block], to)

    def y_copy(k, j):
        slot = wrap(my_slot + k, PEERS)
        to = device_at(lax.div(slot, NC), z, lax.rem(slot, NC))
        return send(sent.at[j, slot], got.at[j, my_slot], ysend.at[j, k], yrecv.at[j, my_slot], to)

    def wait_y(k, j):
        slot = wrap(my_slot + k, PEERS)
        to = device_at(lax.div(slot, NC), z, lax.rem(slot, NC))
        send(sent.at[j, slot], got.at[j, slot], ysend.at[j, k], yrecv.at[j, slot], to).wait_recv()

    def o_copy(k, j):
        slot = wrap(my_slot + k, PEERS)
        to = device_at(lax.div(slot, NC), z, lax.rem(slot, NC))
        return send(sent.at[j, slot], back.at[j, my_slot], osend.at[j, k], orecv.at[j, my_slot], to)

    def wait_o(k, j):
        slot = wrap(my_slot + k, PEERS)
        to = device_at(lax.div(slot, NC), z, lax.rem(slot, NC))
        send(sent.at[j, slot], back.at[j, slot], osend.at[j, k], orecv.at[j, slot], to).wait_recv()

    def direction(j):
        return 1 - 2 * lax.rem(j, 2)

    def z_major(j, s):
        d = direction(j)
        return z_copy(wrap(z - d * s, NZ), j, s, device_at(y, wrap(z + d, NZ), c))

    def z_minor(j, s):
        d = direction(j)
        return z_copy(wrap(z + d * s, NZ), j, 4 + s, device_at(y, wrap(z - d, NZ), c))

    def t_major(s):
        return t_copy(wrap(z - s, NZ), s, device_at(y, wrap(z + 1, NZ), c))

    def t_minor(s):
        return t_copy(wrap(z + s, NZ), 4 + s, device_at(y, wrap(z - 1, NZ), c))

    def build_tables():
        r = lax.broadcasted_iota(jnp.int32, (ALLROWS, TOK), 0)
        group = lax.shift_right_logical(r * 9363, 17)
        within = r - group * CAP
        peer = lax.shift_right_logical(group, 3)
        block = group - peer * NZ
        owner_y = lax.shift_right_logical(peer, 1)
        owner_c = peer - owner_y * NC
        owner = (owner_y * NZ + z) * NC + owner_c
        code = (block * (EXPERTS * CAP) + owner * CAP + within).astype(jnp.float32)

        def one_block(b, carry):
            rows_b = table[b]
            hot = jnp.zeros((ALLROWS, TOK), jnp.float32)
            mixed = jnp.zeros((ALLROWS, TOK), jnp.float32)
            for k in range(6):
                hit = code == jnp.broadcast_to(rows_b[k : k + 1, :], (ALLROWS, TOK))
                hot = jnp.where(hit, 1.0, hot)
                mixed = jnp.where(hit, jnp.broadcast_to(rows_b[8 + k : 9 + k, :], (ALLROWS, TOK)), mixed)
            place_m[:, pl.ds(pl.multiple_of(b * TOK, TOK), TOK)] = hot.astype(jnp.bfloat16)
            mix_m[b] = mixed.T.astype(jnp.bfloat16)
            return carry

        lax.fori_loop(0, NZ, one_block, 0)

    gate_acc[...] = jnp.zeros_like(gate_acc)
    up_acc[...] = jnp.zeros_like(up_acc)

    def dispatch_step(i, carry):
        for s in range(4):
            j = i - s

            @pl.when((j >= 0) & (j < Q))
            def _():
                d = direction(j)
                block = wrap(z - d * s, NZ)
                copy = z_major(j, s)
                if s > 0:
                    z_copy(block, j, s, device_at(y, wrap(z + d, NZ), c)).wait_recv()
                copy.start()
                if s < 3:
                    block2 = wrap(z + d * s, NZ)
                    copy2 = z_minor(j, s)
                    if s > 0:
                        z_copy(block2, j, 4 + s, device_at(y, wrap(z - d, NZ), c)).wait_recv()
                    copy2.start()

        for s in range(4):

            @pl.when(i == s)
            def _():
                copy = t_major(s)
                if s > 0:
                    copy.wait_recv()
                copy.start()
                if s < 3:
                    copy2 = t_minor(s)
                    if s > 0:
                        copy2.wait_recv()
                    copy2.start()

        @pl.when(i == 4)
        def _():
            t_copy(wrap(z - 4, NZ), 0, me).wait_recv()
            t_copy(wrap(z + 3, NZ), 0, me).wait_recv()
            build_tables()

        j = i - 4

        @pl.when((j >= 0) & (j < Q))
        def _():
            d = direction(j)
            z_copy(wrap(z - 4 * d, NZ), j, 0, me).wait_recv()
            z_copy(wrap(z + 3 * d, NZ), j, 0, me).wait_recv()
            block_rows = xs[:, j].reshape(NZ * TOK, width)
            packed = bdot(place_m[...], block_rows).astype(jnp.bfloat16)
            sent[j] = packed.reshape(PEERS, ROWS, width)
            got[j, my_slot] = sent[j, my_slot]

        j2 = i - 6

        @pl.when(j2 >= 0)
        def _():
            @pl.when(j2 == 0)
            def _():
                loads[1].wait()
                loads[2].wait()

            for k in range(1, PEERS):
                wait_y(k, j2)
            x = got[j2].reshape(ALLROWS, width)
            cols = pl.ds(pl.multiple_of(j2 * width, width), width)
            gate_acc[...] += lax.dot_general(x, wg[:, cols], (((1,), (1,)), ((), ())), preferred_element_type=jnp.float32)
            up_acc[...] += lax.dot_general(x, wu[:, cols], (((1,), (1,)), ((), ())), preferred_element_type=jnp.float32)

        @pl.when((j >= 0) & (j < Q))
        def _():
            for k in range(1, PEERS):
                y_copy(k, j).start()

        return carry

    lax.fori_loop(0, Q + 6, dispatch_step, 0)

    g = gate_acc[...]
    act[...] = ((g / (1.0 + jnp.exp(-g))) * up_acc[...]).astype(jnp.bfloat16)
    loads[3].wait()
    loads[4].wait()

    def drain_dispatch(j, carry):
        for s in range(4):
            z_major(j, s).wait_send()
            if s < 3:
                z_minor(j, s).wait_send()
        for k in range(1, PEERS):
            y_copy(k, j).wait_send()
        return carry

    lax.fori_loop(0, Q, drain_dispatch, 0)
    for s in range(4):
        t_major(s).wait_send()
        if s < 3:
            t_minor(s).wait_send()

    def r_major(j, s):
        return send(xs.at[s, j], landed.at[s, j], rsend.at[j, s], rrecv.at[j, s],
                    device_at(y, wrap(z + direction(j), NZ), c))

    def r_minor(j, s):
        return send(xs.at[4 + s, j], landed.at[4 + s, j], rsend.at[j, 4 + s], rrecv.at[j, 4 + s],
                    device_at(y, wrap(z - direction(j), NZ), c))

    def combine_step(i, carry):
        @pl.when(i < Q)
        def _():
            cols = pl.ds(pl.multiple_of(i * width, width), width)
            made = bdot(act[...], wd[:, cols]).astype(jnp.bfloat16)
            sent[i] = made.reshape(PEERS, ROWS, width)
            back[i, my_slot] = sent[i, my_slot]

        jm = i - 2

        @pl.when((jm >= 0) & (jm < Q))
        def _():
            for k in range(1, PEERS):
                wait_o(k, jm)
            rows_in = back[jm].reshape(ALLROWS, width)
            mixed = bdot(mix_m[...].reshape(NZ * TOK, ALLROWS), rows_in)
            part[jm] = mixed.reshape(NZ, TOK, width)

        for s in (3, 2, 1, 0):
            j = i - 2 - s

            @pl.when((j >= 0) & (j < Q))
            def _():
                d = direction(j)
                value = part[j, wrap(z + d * (4 - s), NZ)]
                if s > 0:
                    r_major(j, s - 1).wait_recv()
                    value = value + landed[s - 1, j].astype(jnp.float32)
                xs[s, j] = value.astype(jnp.bfloat16)
                if s < 3:
                    value2 = part[j, wrap(z - d * (3 - s), NZ)]
                    if s > 0:
                        r_minor(j, s - 1).wait_recv()
                        value2 = value2 + landed[4 + s - 1, j].astype(jnp.float32)
                    xs[4 + s, j] = value2.astype(jnp.bfloat16)

        for s in (3, 2, 1, 0):
            j = i - 2 - s

            @pl.when((j >= 0) & (j < Q))
            def _():
                r_major(j, s).start()
                if s < 3:
                    r_minor(j, s).start()

        @pl.when(i < Q)
        def _():
            for k in range(1, PEERS):
                o_copy(k, i).start()

        jf = i - 6

        @pl.when((jf >= 0) & (jf < Q))
        def _():
            r_major(jf, 3).wait_recv()
            r_minor(jf, 2).wait_recv()
            total = part[jf, z] + landed[3, jf].astype(jnp.float32) + landed[6, jf].astype(jnp.float32)
            cols = pl.ds(pl.multiple_of(jf * width, width), width)
            out_ref[:, cols] = (resid[:, cols] + total).astype(jnp.bfloat16)

        return carry

    lax.fori_loop(0, Q + 6, combine_step, 0)

    def drain_combine(j, carry):
        for s in range(4):
            r_major(j, s).wait_send()
            if s < 3:
                r_minor(j, s).wait_send()
        for k in range(1, PEERS):
            o_copy(k, j).wait_send()
        return carry

    lax.fori_loop(0, Q, drain_combine, 0)


def run_experts(nq, resid, ids_t, gates_t, w_gate, w_up, w_down):
    width = nq.shape[2]
    hidden_units, model_width = w_gate.shape
    anywhere = pl.BlockSpec(memory_space=pl.ANY)
    vmem = pl.BlockSpec(memory_space=pltpu.VMEM)
    bf16, f32 = jnp.bfloat16, jnp.float32
    dma = pltpu.SemaphoreType.DMA
    return pl.pallas_call(
        expert_kernel,
        out_shape=jax.ShapeDtypeStruct((TOK, model_width), bf16),
        in_specs=[anywhere, anywhere, vmem, vmem, anywhere, anywhere, anywhere],
        out_specs=vmem,
        scratch_shapes=[
            pltpu.VMEM((NZ, Q, TOK, width), bf16),
            pltpu.VMEM((ALLROWS, NZ * TOK), bf16),
            pltpu.VMEM((NZ, TOK, ALLROWS), bf16),
            pltpu.VMEM((Q, PEERS, ROWS, width), bf16),
            pltpu.VMEM((Q, PEERS, ROWS, width), bf16),
            pltpu.VMEM((ALLROWS, hidden_units), f32),
            pltpu.VMEM((ALLROWS, hidden_units), f32),
            pltpu.VMEM((ALLROWS, hidden_units), bf16),
            pltpu.VMEM((hidden_units, model_width), bf16),
            pltpu.VMEM((hidden_units, model_width), bf16),
            pltpu.VMEM((hidden_units, model_width), bf16),
            pltpu.VMEM((Q, PEERS, ROWS, width), bf16),
            pltpu.VMEM((Q, NZ, TOK, width), f32),
            pltpu.VMEM((7, Q, TOK, width), bf16),
            pltpu.VMEM((TOK, model_width), f32),
            pltpu.VMEM((NZ, 16, TOK), f32),
            dma((5,)),
            dma((Q, 7)), dma((Q, NZ)), dma((Q, PEERS)), dma((Q, PEERS)), dma((Q, PEERS)), dma((Q, PEERS)),
            dma((Q, 7)), dma((Q, 7)), dma((7,)), dma((NZ,)),
        ],
        compiler_params=pltpu.CompilerParams(
            collective_id=1, has_side_effects=True, vmem_limit_bytes=60 * 1024 * 1024
        ),
        name="experts",
    )(nq, resid, ids_t, gates_t, w_gate, w_up, w_down)


HEADS = 8
NX = 4
SEGKEYS = NY * NZ * NC


def attend_kernel(
    lat_hbm, q_ref, mem_ref, len_ref, hid_ref, gain_ref, wuv_hbm, wout_hbm, nq_ref, resid_ref,
    keys, qrows, acc, top, total, wuv, wout,
    load_sem, ksend, krecv, psend, precv, wsend, wrecv, wpsend, wprecv,
):
    me, y, z, c = place()
    x = lax.axis_index("dp")
    pos = lat_hbm.shape[1]
    lat = lat_hbm.shape[2]
    rows = HEADS * pos
    partner = device_at(y, z, 1 - c)
    own_start = pl.multiple_of(me * pos, pos)

    loads = [
        pltpu.make_async_copy(lat_hbm.at[0], keys.at[0, pl.ds(own_start, pos)], load_sem.at[0]),
        pltpu.make_async_copy(lat_hbm.at[1], keys.at[1, pl.ds(own_start, pos)], load_sem.at[1]),
        pltpu.make_async_copy(wout_hbm, wout.at[x], load_sem.at[2]),
        pltpu.make_async_copy(wuv_hbm, wuv.at[x], load_sem.at[3]),
    ]
    for load in loads:
        load.start()

    barrier = pltpu.get_barrier_semaphore()
    mesh_id = pl.DeviceIdType.MESH
    expert_ids = [
        device_at(y, wrap(z + 1, NZ), c), device_at(y, wrap(z - 1, NZ), c),
        device_at(wrap(y + 1, NY), z, c), device_at(wrap(y - 1, NY), z, c), partner,
    ]
    for dev in expert_ids:
        pl.semaphore_signal(barrier, inc=1, device_id={"expert": dev}, device_id_type=mesh_id)
    for dev in (wrap(x + 1, NX), wrap(x - 1, NX)):
        pl.semaphore_signal(barrier, inc=1, device_id={"dp": dev}, device_id_type=mesh_id)

    def key_block(s, by, bz, bc):
        return keys.at[s, pl.ds(pl.multiple_of(device_at(by, bz, bc) * pos, pos), pos)]

    def k_copy(s, role, by, bz, to):
        ref = key_block(s, by, bz, c)
        block = by * NZ + bz
        return send(ref, ref, ksend.at[s, role, block], krecv.at[s, block], to)

    def p_copy(s, by, bz, bc):
        ref = key_block(s, by, bz, bc)
        block = by * NZ + bz
        return send(ref, ref, psend.at[s, block], precv.at[s, block], partner)

    def w_pieces(bx, bc):
        half = wout.shape[1] // 2
        sub = half // 2
        first = wout.at[bx, pl.ds(pl.multiple_of(bc * half, half), sub)]
        second = wout.at[bx, pl.ds(pl.multiple_of(bc * half + sub, sub), sub)]
        return [first, second, wuv.at[bx, bc]]

    def w_copy(bx, piece, role, to):
        ref = w_pieces(bx, c)[piece]
        return pltpu.make_async_remote_copy(
            src_ref=ref, dst_ref=ref, send_sem=wsend.at[role, piece], recv_sem=wrecv.at[bx, piece],
            device_id={"dp": to}, device_id_type=mesh_id,
        )

    def wp_copy(bx, piece, bc):
        ref = w_pieces(bx, bc)[piece]
        return send(ref, ref, wpsend.at[bx, piece], wprecv.at[bx, piece], partner)

    rounds = [[] for _ in range(8)]
    sends = []

    def add_send(t, make):
        sends.append(make)
        rounds[t].append(lambda: make().start())

    def add_wait(t, make):
        rounds[t].append(lambda: make().wait_recv())

    def dir_of(v):
        return 1 - 2 * lax.rem(v, 2)

    def arrived_everywhere(s, t, by, bz, second):
        add_send(t, lambda: p_copy(s, by, bz, c))
        if second is not None:
            second(t, by, bz)

    def along(s, t, by, bz, axis, d, first_role, then):
        n = NZ if axis == "z" else NY
        major, minor = n // 2, n - 1 - n // 2

        def to(k):
            return device_at(y, wrap(z + k, NZ), c) if axis == "z" else device_at(wrap(y + k, NY), z, c)

        def block(k):
            return (by, wrap(bz + k, NZ)) if axis == "z" else (wrap(by + k, NY), bz)

        add_send(t, lambda: k_copy(s, first_role, by, bz, to(d)))
        add_send(t, lambda: k_copy(s, first_role + 1, by, bz, to(-d)))
        for h in range(1, major + 1):
            b = block(-d * h)
            add_wait(t + h, lambda b=b: k_copy(s, first_role, *b, me))
            if h < major:
                add_send(t + h, lambda b=b: k_copy(s, first_role, *b, to(d)))
            arrived_everywhere(s, t + h, *b, then)
            if h <= minor:
                b2 = block(d * h)
                add_wait(t + h, lambda b2=b2: k_copy(s, first_role, *b2, me))
                if h < minor:
                    add_send(t + h, lambda b2=b2: k_copy(s, first_role + 1, *b2, to(-d)))
                arrived_everywhere(s, t + h, *b2, then)

    second_a = lambda t, by, bz: along(0, t, by, bz, "y", dir_of(bz), 2, None)
    second_b = lambda t, by, bz: along(1, t, by, bz, "z", dir_of(by), 2, None)
    arrived_everywhere(1, 0, y, z, second_b)
    along(1, 0, y, z, "y", 1, 0, second_b)
    arrived_everywhere(0, 0, y, z, second_a)
    along(0, 0, y, z, "z", 1, 0, second_a)

    for piece in (2, 0, 1):
        add_send(0, lambda piece=piece: w_copy(x, piece, 0, wrap(x + 1, NX)))
        add_send(0, lambda piece=piece: w_copy(x, piece, 1, wrap(x - 1, NX)))
    before, after, far = wrap(x - 1, NX), wrap(x + 1, NX), wrap(x + 2, NX)
    for piece in (2, 0, 1):
        for bx in (before, after):
            add_wait(5, lambda bx=bx, piece=piece: w_copy(bx, piece, 0, x))
            add_send(5, lambda bx=bx, piece=piece: wp_copy(bx, piece, c))
        if piece == 1:
            add_send(5, lambda: w_copy(after, 1, 3, before))
        else:
            add_send(5, lambda piece=piece: w_copy(before, piece, 2, after))
    for piece in (2, 0, 1):
        add_wait(7, lambda piece=piece: w_copy(far, piece, 0, x))
        add_send(7, lambda piece=piece: wp_copy(far, piece, c))

    scale = score_scale
    for s in range(2):
        for h in range(HEADS):
            qrows[s, h * pos : (h + 1) * pos, :] = q_ref[s, :, h * lat : (h + 1) * lat]
    row_pos = me * pos + lax.bitwise_and(lax.broadcasted_iota(jnp.int32, (rows, 1), 0), pos - 1)
    contract_last = (((1,), (1,)), ((), ()))
    for s in range(2):
        k = mem_ref[s]
        sc = lax.dot_general(qrows[s], k, contract_last, preferred_element_type=jnp.float32) * scale
        m = jnp.max(sc, axis=1, keepdims=True)
        p = jnp.exp(sc - m)
        top[s] = jnp.broadcast_to(m, (rows, 128))
        total[s] = jnp.broadcast_to(jnp.sum(p, axis=1, keepdims=True), (rows, 128))
        acc[s] = bdot(p.astype(jnp.bfloat16), k)

    def fold(s, bz):
        run = NC * pos
        k = jnp.concatenate(
            [keys[s, pl.ds(pl.multiple_of(device_at(by, bz, 0) * pos, run), run), :] for by in range(NY)], axis=0
        )
        count = NY * run
        sc = lax.dot_general(qrows[s], k, contract_last, preferred_element_type=jnp.float32) * scale
        lane = lax.broadcasted_iota(jnp.int32, (1, count), 1)
        key_pos = lax.shift_right_logical(lane, 7) * (NZ * run) + bz * run + lax.bitwise_and(lane, run - 1)
        limit = jnp.minimum(row_pos + 1, len_ref[s])
        sc = jnp.where(key_pos < limit, sc, -jnp.inf)
        old = top[s]
        new = jnp.maximum(old, jnp.max(sc, axis=1, keepdims=True))
        factor = jnp.exp(old - new)
        p = jnp.exp(sc - new[:, 0:1])
        top[s] = new
        total[s] = total[s] * factor + jnp.sum(p, axis=1, keepdims=True)
        acc[s] = acc[s] * factor[:, 0:1] + bdot(p.astype(jnp.bfloat16), k)

    pl.semaphore_wait(barrier, len(expert_ids) + 2)
    for load in loads:
        load.wait()

    def round_step(t, carry):
        for r in range(8):

            @pl.when(t == r)
            def _():
                for act in rounds[r]:
                    act()

        u = t - 3

        @pl.when(u >= 0)
        def _():
            count = jnp.where((u == 0) | (u == 4), 1, 2)

            def piece(v, carry2):
                bz = wrap(z + u * (1 - 2 * v), NZ)
                for by in range(NY):
                    for s in range(2):
                        p_copy(s, by, bz, 1 - c).wait_recv()
                for s in range(2):
                    fold(s, bz)
                return carry2

            lax.fori_loop(0, count, piece, 0)

        return carry

    lax.fori_loop(0, 8, round_step, 0)

    for bx in (before, after, far):
        for piece in range(3):
            wp_copy(bx, piece, 1 - c).wait_recv()

    heads = []
    per = wuv.shape[1]
    for h in range(HEADS):
        part = []
        for s in range(2):
            one = slice(h * pos, (h + 1) * pos)
            part.append((acc[s, one, :] / total[s, one, 0:1]).astype(jnp.bfloat16))
        mixed = jnp.concatenate(part, axis=0)
        heads.append(bdot(mixed, wuv[h // per, h % per]).astype(jnp.bfloat16))
    values = jnp.concatenate(heads, axis=1)
    width = nq_ref.shape[2]
    squares = jnp.zeros((TOK, 1), jnp.float32)
    deep = wout.shape[0] * wout.shape[1]
    for j in range(Q):
        cols = slice(j * width, (j + 1) * width)
        res = bdot(values, wout[:, :, cols].reshape(deep, width)) + hid_ref[:, cols].astype(jnp.float32)
        resid_ref[:, cols] = res
        squares = squares + jnp.sum(res * res, axis=1, keepdims=True)
    rs = lax.rsqrt(squares / (Q * width) + norm_eps)
    for j in range(Q):
        cols = slice(j * width, (j + 1) * width)
        nq_ref[j] = (resid_ref[:, cols] * rs * gain_ref[:, cols].astype(jnp.float32)).astype(jnp.bfloat16)

    for make in sends:
        make().wait_send()


def run_attention(lat, q, mem, lengths, hid, gain, w_uv, w_out):
    anywhere = pl.BlockSpec(memory_space=pl.ANY)
    vmem = pl.BlockSpec(memory_space=pltpu.VMEM)
    bf16, f32 = jnp.bfloat16, jnp.float32
    dma = pltpu.SemaphoreType.DMA
    seqs, pos, lat_dim = lat.shape
    rows = HEADS * pos
    model_width = hid.shape[1]
    blocks = NY * NZ
    return pl.pallas_call(
        attend_kernel,
        out_shape=(
            jax.ShapeDtypeStruct((Q, TOK, model_width // Q), bf16),
            jax.ShapeDtypeStruct((TOK, model_width), f32),
        ),
        in_specs=[anywhere, vmem, vmem, pl.BlockSpec(memory_space=pltpu.SMEM), vmem, vmem, anywhere, anywhere],
        out_specs=(vmem, vmem),
        scratch_shapes=[
            pltpu.VMEM((seqs, SEGKEYS * pos, lat_dim), bf16),
            pltpu.VMEM((seqs, rows, lat_dim), bf16),
            pltpu.VMEM((seqs, rows, lat_dim), f32),
            pltpu.VMEM((seqs, rows, 128), f32),
            pltpu.VMEM((seqs, rows, 128), f32),
            pltpu.VMEM((NX,) + w_uv.shape, bf16),
            pltpu.VMEM((NX,) + w_out.shape, bf16),
            dma((4,)),
            dma((seqs, 4, blocks)), dma((seqs, blocks)), dma((seqs, blocks)), dma((seqs, blocks)),
            dma((4, 3)), dma((NX, 3)), dma((NX, 3)), dma((NX, 3)),
        ],
        compiler_params=pltpu.CompilerParams(
            collective_id=0, has_side_effects=True, vmem_limit_bytes=60 * 1024 * 1024
        ),
        name="attend",
    )(lat, q, mem, lengths, hid, gain, w_uv, w_out)


def shards(
    hidden,
    queries,
    latents,
    mem_latents,
    lengths,
    ids,
    gates,
    norm_gain,
    w_uv,
    w_out,
    w_gate,
    w_up,
    w_down,
):
    _, local_len, seq_count, model_width = hidden.shape
    lat = jnp.swapaxes(latents[0], 0, 1)
    q = jnp.swapaxes(queries[0], 0, 1)
    mem = jnp.swapaxes(mem_latents[0], 0, 1)
    hid = jnp.swapaxes(hidden[0], 0, 1).reshape(TOK, model_width)
    ids_t = jnp.pad(ids[0].transpose(2, 1, 0).reshape(-1, TOK), ((0, 2), (0, 0)), constant_values=-1)
    gates_t = jnp.pad(gates[0].transpose(2, 1, 0).reshape(-1, TOK).astype(jnp.float32), ((0, 2), (0, 0)))
    nq, resid = run_attention(lat, q, mem, lengths[0], hid, norm_gain[None], w_uv, w_out)
    out = run_experts(
        nq, resid, ids_t, gates_t, jnp.swapaxes(w_gate[0], 0, 1), jnp.swapaxes(w_up[0], 0, 1), w_down[0]
    )
    return jnp.swapaxes(out.reshape(seq_count, local_len, model_width), 0, 1)[None]


def solution(mesh):
    return jax.shard_map(
        shards,
        mesh=mesh,
        in_specs=(
            P("dp", "expert", None, None),
            P("dp", "expert", None, None),
            P("dp", "expert", None, None),
            P("dp", None, None, None),
            P("dp", None),
            P("dp", "expert", None, None),
            P("dp", "expert", None, None),
            P(),
            P("dp", None, None),
            P("dp", None),
            P("expert", None, None),
            P("expert", None, None),
            P("expert", None, None),
        ),
        out_specs=P("dp", "expert", None, None),
        check_vma=False,
    )
```

```python
import jax
import jax.numpy as jnp
from jax import lax
from jax.experimental import pallas as pl
from jax.experimental.pallas import tpu as pltpu
from jax.sharding import PartitionSpec as P

score_scale = 192.0 ** (-0.5)
norm_eps = 1e-06


NY, NZ, NC = 4, 8, 2
Q = 8
ADVANCE = 1
HOP1, NEAR_AT, HOP2, HOP3 = 1, 2, 2, 3
FAR_AT = HOP3 + 1
FFN_NEAR = NEAR_AT + 3
FFN_FAR = FAR_AT + 2
RET_NEAR = 2
MIX_FAR, MIX_NEAR = 2, RET_NEAR + 2
SUM1 = MIX_FAR + 1
SUM2 = MIX_NEAR
SUM3 = SUM2 + 1
LAST = SUM3 + 1
TOK = 128
CAP = 14
EXPERTS = 64
PEERS = NY * NC
ROWS = NZ * CAP
ALLROWS = PEERS * ROWS
NEAR = 4
REL = (0, -1, 1, -2, 2, -3, 3, 4)
SLOT = {r: i for i, r in enumerate(REL)}
GROUPS = NZ // NEAR
GROWS = NEAR * CAP
HALF = PEERS * GROWS


def place():
    me = lax.axis_index("expert")
    c = lax.rem(me, NC)
    z = lax.rem(lax.div(me, NC), NZ)
    y = lax.div(me, NC * NZ)
    return me, y, z, c


def device_at(y, z, c):
    return (y * NZ + z) * NC + c


def wrap(v, n):
    return lax.rem(v + 2 * n, n)


def send(src, dst, ssem, rsem, to):
    return pltpu.make_async_remote_copy(
        src_ref=src,
        dst_ref=dst,
        send_sem=ssem,
        recv_sem=rsem,
        device_id={"expert": to},
        device_id_type=pl.DeviceIdType.MESH,
    )


def bdot(a, b):
    return jnp.dot(a, b, preferred_element_type=jnp.float32)


def expert_kernel(
    nq_hbm, resid_hbm, ids_ref, gates_ref, wg_hbm, wu_hbm, wd_hbm, out_ref,
    xs, place_m, mix_m, sent, got, gate_acc, up_acc, act, wg, wu, wd, back, part, landed, resid, table,
    load_sem, zsend, zrecv, ysend, yrecv, osend, orecv, rsend, rrecv, tsend, trecv,
):
    width = xs.shape[3]
    me, y, z, c = place()
    my_slot = y * NC + c
    right = device_at(y, wrap(z + 1, NZ), c)
    left = device_at(y, wrap(z - 1, NZ), c)

    loads = [
        pltpu.make_async_copy(nq_hbm, xs.at[0], load_sem.at[0]),
        pltpu.make_async_copy(wg_hbm, wg, load_sem.at[1]),
        pltpu.make_async_copy(wu_hbm, wu, load_sem.at[2]),
        pltpu.make_async_copy(wd_hbm, wd, load_sem.at[3]),
        pltpu.make_async_copy(resid_hbm, resid, load_sem.at[4]),
    ]
    for load in loads:
        load.start()

    barrier = pltpu.get_barrier_semaphore()

    def peer(k):
        slot = wrap(my_slot + k, PEERS)
        return slot, device_at(lax.div(slot, NC), z, lax.rem(slot, NC))

    partners = [peer(k)[1] for k in range(1, PEERS)] + [right, left]
    for dev in partners:
        pl.semaphore_signal(barrier, inc=1, device_id={"expert": dev}, device_id_type=pl.DeviceIdType.MESH)

    expert_iota = lax.broadcasted_iota(jnp.int32, (EXPERTS, TOK), 0)
    hits = []
    named = jnp.zeros((EXPERTS, TOK), jnp.float32)
    for k in range(6):
        hit = expert_iota == jnp.broadcast_to(ids_ref[k : k + 1, :], (EXPERTS, TOK))
        hits.append(hit)
        named = named + jnp.where(hit, 1.0, 0.0)
    earlier = lax.broadcasted_iota(jnp.int32, (TOK, TOK), 0) < lax.broadcasted_iota(jnp.int32, (TOK, TOK), 1)
    before = bdot(named.astype(jnp.bfloat16), jnp.where(earlier, 1.0, 0.0).astype(jnp.bfloat16))
    expert_base = (expert_iota * CAP).astype(jnp.float32)
    rows = []
    for k in range(6):
        rows.append(jnp.sum(jnp.where(hits[k], before + expert_base, 0.0), axis=0, keepdims=True))
    filler = jnp.full((2, TOK), -1.0, jnp.float32)
    table[0] = jnp.concatenate(rows + [filler, gates_ref[...].astype(jnp.float32), filler], axis=0)

    gate_acc[...] = jnp.zeros_like(gate_acc)
    up_acc[...] = jnp.zeros_like(up_acc)

    pl.semaphore_wait(barrier, len(partners))
    loads[0].wait()

    def z_hop(j, h, sign):
        src = SLOT[-sign * h]
        dst = SLOT[-sign * (h + 1)] if h < 3 else SLOT[4]
        sem = 6 if h == 3 else h + (0 if sign > 0 else 3)
        return send(xs.at[src, j], xs.at[dst, j], zsend.at[j, sem], zrecv.at[j, dst], right if sign > 0 else left)

    def t_hop(h, sign):
        src = SLOT[-sign * h]
        dst = SLOT[-sign * (h + 1)] if h < 3 else SLOT[4]
        sem = 6 if h == 3 else h + (0 if sign > 0 else 3)
        return send(table.at[src], table.at[dst], tsend.at[sem], trecv.at[dst], right if sign > 0 else left)

    def z_here(j, slot):
        send(xs.at[slot, j], xs.at[slot, j], zsend.at[j, 0], zrecv.at[j, slot], right).wait_recv()

    def t_here(slot):
        send(table.at[slot], table.at[slot], tsend.at[0], trecv.at[slot], right).wait_recv()

    def y_copy(k, j, g):
        slot, to = peer(k)
        return send(sent.at[j, g, slot], got.at[j, g, my_slot], ysend.at[g, j, k], yrecv.at[g, j, my_slot], to)

    def y_here(k, j, g):
        slot, to = peer(k)
        send(sent.at[j, g, slot], got.at[j, g, slot], ysend.at[g, j, k], yrecv.at[g, j, slot], to).wait_recv()

    def o_copy(k, j, g):
        slot, to = peer(k)
        return send(sent.at[j, g, slot], back.at[j, g, my_slot], osend.at[g, j, k], orecv.at[g, j, my_slot], to)

    def o_here(k, j, g):
        slot, to = peer(k)
        send(sent.at[j, g, slot], back.at[j, g, slot], osend.at[g, j, k], orecv.at[g, j, slot], to).wait_recv()

    def parity(j):
        return lax.rem(z + j, 2)

    def build_tables(g):
        r = lax.broadcasted_iota(jnp.int32, (HALF, TOK), 0)
        group = lax.shift_right_logical(r * 9363, 17)
        within = r - group * CAP
        owner_slot = lax.shift_right_logical(group, 2)
        near = group - owner_slot * NEAR
        owner_y = lax.shift_right_logical(owner_slot, 1)
        owner_c = owner_slot - owner_y * NC
        owner = (owner_y * NZ + z) * NC + owner_c
        base = owner * CAP + within

        def one_block(b, carry):
            code = jnp.where(near == b, base, -7).astype(jnp.float32)
            rows_b = table[g * NEAR + b]
            hot = jnp.zeros((HALF, TOK), jnp.float32)
            mixed = jnp.zeros((HALF, TOK), jnp.float32)
            for k in range(6):
                hit = code == jnp.broadcast_to(rows_b[k : k + 1, :], (HALF, TOK))
                hot = jnp.where(hit, 1.0, hot)
                mixed = jnp.where(hit, jnp.broadcast_to(rows_b[8 + k : 9 + k, :], (HALF, TOK)), mixed)
            place_m[g, :, pl.ds(pl.multiple_of(b * TOK, TOK), TOK)] = hot.astype(jnp.bfloat16)
            mix_m[g, pl.ds(pl.multiple_of(b * TOK, TOK), TOK), :] = mixed.T.astype(jnp.bfloat16)
            return carry

        lax.fori_loop(0, NEAR, one_block, 0)

    def on(cond, f):
        pl.when(cond)(f)

    def valid(j):
        return (j >= 0) & (j < Q)

    def dispatch_step(i, carry):
        def own(j):
            z_hop(j, 0, 1).start()
            z_hop(j, 0, -1).start()

        @pl.when(i == 0)
        def _():
            t_hop(0, 1).start()
            t_hop(0, -1).start()
            for j in range(ADVANCE):
                own(j)

        on(i + ADVANCE < Q, lambda: own(i + ADVANCE))

        def forward(j, h, hop, here):
            here(j, SLOT[-h])
            if h < 3:
                hop(j, h, 1).start()
            here(j, SLOT[h])
            if h < 3:
                hop(j, h, -1).start()
            else:
                on(parity(j) == 1, lambda: hop(j, 3, 1).start())
                on(parity(j) == 0, lambda: hop(j, 3, -1).start())

        def compact(j, g):
            block_rows = xs[g * NEAR : (g + 1) * NEAR, j].reshape(NEAR * TOK, width)
            packed = bdot(place_m[g], block_rows).astype(jnp.bfloat16)
            sent[j, g] = packed.reshape(PEERS, GROWS, width)
            got[j, g, my_slot] = sent[j, g, my_slot]

        def ship(j, g):
            for k in range(1, PEERS):
                y_copy(k, j, g).start()

        def feed(j, g):
            for k in range(1, PEERS):
                y_here(k, j, g)
            x = got[j, g].reshape(HALF, width)
            cols = pl.ds(pl.multiple_of(j * width, width), width)
            last = (((1,), (1,)), ((), ()))
            gate_acc[g] += lax.dot_general(x, wg[:, cols], last, preferred_element_type=jnp.float32)
            up_acc[g] += lax.dot_general(x, wu[:, cols], last, preferred_element_type=jnp.float32)

        @pl.when(valid(i - HOP1))
        def _():
            forward(i - HOP1, 1, z_hop, z_here)

        for h in (1, 2, 3):
            on(i == h, lambda: forward(0, h, lambda j, k, sign: t_hop(k, sign), lambda j, slot: t_here(slot)))

        jn, j2, j3, jf = i - NEAR_AT, i - HOP2, i - HOP3, i - FAR_AT

        @pl.when(valid(jn))
        def _():
            z_here(jn, SLOT[-2])

        @pl.when(valid(j2))
        def _():
            z_hop(j2, 2, 1).start()
            z_here(j2, SLOT[2])
            z_hop(j2, 2, -1).start()

        on(valid(j3), lambda: forward(j3, 3, z_hop, z_here))
        on(i == 2, lambda: build_tables(0))

        @pl.when(i == 4)
        def _():
            t_here(SLOT[4])
            build_tables(1)

        on(valid(jn), lambda: compact(jn, 0))

        @pl.when(valid(jf))
        def _():
            z_here(jf, SLOT[4])
            compact(jf, 1)

        on(valid(jn), lambda: ship(jn, 0))

        @pl.when(i == FFN_NEAR)
        def _():
            loads[1].wait()
            loads[2].wait()

        on(valid(i - FFN_NEAR), lambda: feed(i - FFN_NEAR, 0))
        on(valid(jf), lambda: ship(jf, 1))
        on(valid(i - FFN_FAR), lambda: feed(i - FFN_FAR, 1))
        return carry

    lax.fori_loop(0, Q + FFN_FAR, dispatch_step, 0)

    g = gate_acc[...]
    act[...] = ((g / (1.0 + jnp.exp(-g))) * up_acc[...]).astype(jnp.bfloat16)
    loads[3].wait()
    loads[4].wait()

    def drain_dispatch(j, carry):
        for h in range(3):
            z_hop(j, h, 1).wait_send()
            z_hop(j, h, -1).wait_send()
        z_hop(j, 3, 1).wait_send()
        for g in range(GROUPS):
            for k in range(1, PEERS):
                y_copy(k, j, g).wait_send()
        return carry

    lax.fori_loop(0, Q, drain_dispatch, 0)
    for h in range(3):
        t_hop(h, 1).wait_send()
        t_hop(h, -1).wait_send()
    t_hop(3, 1).wait_send()

    def r_copy(j, k, to):
        return send(xs.at[k, j], landed.at[k, j], rsend.at[j, k], rrecv.at[j, k], to)

    def r_here(j, k):
        r_copy(j, k, right).wait_recv()

    def wide(j, k):
        return landed[k, j].astype(jnp.float32)

    def combine_step(i, carry):
        def make(j, g):
            cols = pl.ds(pl.multiple_of(j * width, width), width)
            made = bdot(act[g], wd[:, cols]).astype(jnp.bfloat16)
            sent[j, g] = made.reshape(PEERS, GROWS, width)
            back[j, g, my_slot] = sent[j, g, my_slot]

        def mix(j, g):
            for k in range(1, PEERS):
                o_here(k, j, g)
            mixed = bdot(mix_m[g], back[j, g].reshape(HALF, width))
            part[j, g * NEAR : (g + 1) * NEAR] = mixed.reshape(NEAR, TOK, width)

        def ship_back(j, g):
            for k in range(1, PEERS):
                o_copy(k, j, g).start()

        on(i < Q, lambda: make(i, 1))
        on(valid(i - RET_NEAR), lambda: make(i - RET_NEAR, 0))
        j0, j1, j2, j3, j4 = i - MIX_FAR, i - SUM1, i - SUM2, i - SUM3, i - LAST

        @pl.when(valid(j0))
        def _():
            mix(j0, 1)
            xs[0, j0] = part[j0, SLOT[4]].astype(jnp.bfloat16)

        @pl.when(valid(j1))
        def _():
            r_here(j1, 0)
            odd = (parity(j1) == 1).astype(jnp.float32)
            arrived = wide(j1, 0)
            xs[1, j1] = (part[j1, SLOT[3]] + arrived * odd).astype(jnp.bfloat16)
            xs[4, j1] = (part[j1, SLOT[-3]] + arrived * (1.0 - odd)).astype(jnp.bfloat16)

        on(i < Q, lambda: ship_back(i, 1))
        on(valid(i - RET_NEAR), lambda: ship_back(i - RET_NEAR, 0))

        @pl.when(valid(j0))
        def _():
            on(parity(j0) == 0, lambda: r_copy(j0, 0, right).start())
            on(parity(j0) == 1, lambda: r_copy(j0, 0, left).start())

        on(valid(i - MIX_NEAR), lambda: mix(i - MIX_NEAR, 0))

        def add_on(j, s):
            r_here(j, s - 1)
            xs[s, j] = (part[j, SLOT[4 - s]] + wide(j, s - 1)).astype(jnp.bfloat16)
            r_here(j, s + 2)
            xs[s + 3, j] = (part[j, SLOT[s - 4]] + wide(j, s + 2)).astype(jnp.bfloat16)

        def pass_on(j, s):
            r_copy(j, s, right).start()
            r_copy(j, s + 3, left).start()

        on(valid(j1), lambda: pass_on(j1, 1))
        on(valid(j3), lambda: add_on(j3, 3))
        on(valid(j2), lambda: add_on(j2, 2))
        on(valid(j3), lambda: pass_on(j3, 3))
        on(valid(j2), lambda: pass_on(j2, 2))

        @pl.when(valid(j4))
        def _():
            r_here(j4, 3)
            r_here(j4, 6)
            total = part[j4, 0] + wide(j4, 3) + wide(j4, 6)
            cols = pl.ds(pl.multiple_of(j4 * width, width), width)
            final = (resid[:, cols] + total).astype(jnp.bfloat16)
            for s in range(2):
                out_ref[:, s, cols] = final[s * (TOK // 2) : (s + 1) * (TOK // 2)]

        return carry

    lax.fori_loop(0, Q + LAST, combine_step, 0)

    def drain_combine(j, carry):
        for k in range(7):
            r_copy(j, k, right).wait_send()
        for g in range(GROUPS):
            for k in range(1, PEERS):
                o_copy(k, j, g).wait_send()
        return carry

    lax.fori_loop(0, Q, drain_combine, 0)


def run_experts(nq, resid, ids_t, gates_t, w_gate, w_up, w_down):
    width = nq.shape[2]
    hidden_units, model_width = w_gate.shape
    anywhere = pl.BlockSpec(memory_space=pl.ANY)
    vmem = pl.BlockSpec(memory_space=pltpu.VMEM)
    bf16, f32 = jnp.bfloat16, jnp.float32
    dma = pltpu.SemaphoreType.DMA
    return pl.pallas_call(
        expert_kernel,
        out_shape=jax.ShapeDtypeStruct((TOK // 2, 2, model_width), bf16),
        in_specs=[anywhere, anywhere, vmem, vmem, anywhere, anywhere, anywhere],
        out_specs=vmem,
        scratch_shapes=[
            pltpu.VMEM((NZ, Q, TOK, width), bf16),
            pltpu.VMEM((GROUPS, HALF, NEAR * TOK), bf16),
            pltpu.VMEM((GROUPS, NEAR * TOK, HALF), bf16),
            pltpu.VMEM((Q, GROUPS, PEERS, GROWS, width), bf16),
            pltpu.VMEM((Q, GROUPS, PEERS, GROWS, width), bf16),
            pltpu.VMEM((GROUPS, HALF, hidden_units), f32),
            pltpu.VMEM((GROUPS, HALF, hidden_units), f32),
            pltpu.VMEM((GROUPS, HALF, hidden_units), bf16),
            pltpu.VMEM((hidden_units, model_width), bf16),
            pltpu.VMEM((hidden_units, model_width), bf16),
            pltpu.VMEM((hidden_units, model_width), bf16),
            pltpu.VMEM((Q, GROUPS, PEERS, GROWS, width), bf16),
            pltpu.VMEM((Q, NZ, TOK, width), f32),
            pltpu.VMEM((7, Q, TOK, width), bf16),
            pltpu.VMEM((TOK, model_width), f32),
            pltpu.VMEM((NZ, 16, TOK), f32),
            dma((5,)),
            dma((Q, 7)), dma((Q, NZ)), dma((GROUPS, Q, PEERS)), dma((GROUPS, Q, PEERS)), dma((GROUPS, Q, PEERS)), dma((GROUPS, Q, PEERS)),
            dma((Q, 7)), dma((Q, 7)), dma((7,)), dma((NZ,)),
        ],
        compiler_params=pltpu.CompilerParams(
            collective_id=1, has_side_effects=True, vmem_limit_bytes=60 * 1024 * 1024
        ),
        name="experts",
    )(nq, resid, ids_t, gates_t, w_gate, w_up, w_down)


HEADS = 8
NX = 4
SEGKEYS = NY * NZ * NC


def attend_kernel(
    lat_hbm, q_ref, mem_ref, len_ref, hid_ref, gain_ref, wuv_hbm, wout_hbm, nq_ref, resid_ref,
    keys, qrows, acc, top, total, wuv, wout,
    load_sem, ksend, krecv, psend, precv, wsend, wrecv, wpsend, wprecv,
):
    me, y, z, c = place()
    x = lax.axis_index("dp")
    pos = lat_hbm.shape[0]
    lat = lat_hbm.shape[2]
    rows = HEADS * pos
    partner = device_at(y, z, 1 - c)
    own_start = pl.multiple_of(me * pos, pos)

    loads = [
        pltpu.make_async_copy(wout_hbm, wout.at[x], load_sem.at[2]),
        pltpu.make_async_copy(wuv_hbm, wuv.at[x], load_sem.at[3]),
    ]
    for load in loads:
        load.start()
    for s in range(2):
        keys[s, pl.ds(own_start, pos), :] = lat_hbm[:, s, :]

    barrier = pltpu.get_barrier_semaphore()
    mesh_id = pl.DeviceIdType.MESH
    expert_ids = [
        device_at(y, wrap(z + 1, NZ), c), device_at(y, wrap(z - 1, NZ), c),
        device_at(wrap(y + 1, NY), z, c), device_at(wrap(y - 1, NY), z, c), partner,
    ]
    for dev in expert_ids:
        pl.semaphore_signal(barrier, inc=1, device_id={"expert": dev}, device_id_type=mesh_id)
    for dev in (wrap(x + 1, NX), wrap(x - 1, NX)):
        pl.semaphore_signal(barrier, inc=1, device_id={"dp": dev}, device_id_type=mesh_id)

    def key_block(s, by, bz, bc):
        return keys.at[s, pl.ds(pl.multiple_of(device_at(by, bz, bc) * pos, pos), pos)]

    def k_copy(s, role, by, bz, to):
        ref = key_block(s, by, bz, c)
        block = by * NZ + bz
        return send(ref, ref, ksend.at[s, role, block], krecv.at[s, block], to)

    def p_copy(s, by, bz, bc):
        ref = key_block(s, by, bz, bc)
        block = by * NZ + bz
        return send(ref, ref, psend.at[s, block], precv.at[s, block], partner)

    def w_pieces(bx, bc):
        half = wout.shape[1] // 2
        sub = half // 2
        first = wout.at[bx, pl.ds(pl.multiple_of(bc * half, half), sub)]
        second = wout.at[bx, pl.ds(pl.multiple_of(bc * half + sub, sub), sub)]
        return [first, second, wuv.at[bx, bc]]

    def w_copy(bx, piece, role, to):
        ref = w_pieces(bx, c)[piece]
        return pltpu.make_async_remote_copy(
            src_ref=ref, dst_ref=ref, send_sem=wsend.at[role, piece], recv_sem=wrecv.at[bx, piece],
            device_id={"dp": to}, device_id_type=mesh_id,
        )

    def wp_copy(bx, piece, bc):
        ref = w_pieces(bx, bc)[piece]
        return send(ref, ref, wpsend.at[bx, piece], wprecv.at[bx, piece], partner)

    rounds = [[] for _ in range(8)]
    sends = []

    def add_send(t, make):
        sends.append(make)
        rounds[t].append(lambda: make().start())

    def add_wait(t, make):
        rounds[t].append(lambda: make().wait_recv())

    def dir_of(v):
        return 1 - 2 * lax.rem(v, 2)

    def arrived_everywhere(s, t, by, bz, second):
        add_send(t, lambda: p_copy(s, by, bz, c))
        if second is not None:
            second(t, by, bz)

    def along(s, t, by, bz, axis, d, first_role, then):
        n = NZ if axis == "z" else NY
        major, minor = n // 2, n - 1 - n // 2

        def to(k):
            return device_at(y, wrap(z + k, NZ), c) if axis == "z" else device_at(wrap(y + k, NY), z, c)

        def block(k):
            return (by, wrap(bz + k, NZ)) if axis == "z" else (wrap(by + k, NY), bz)

        add_send(t, lambda: k_copy(s, first_role, by, bz, to(d)))
        add_send(t, lambda: k_copy(s, first_role + 1, by, bz, to(-d)))
        for h in range(1, major + 1):
            b = block(-d * h)
            add_wait(t + h, lambda b=b: k_copy(s, first_role, *b, me))
            if h < major:
                add_send(t + h, lambda b=b: k_copy(s, first_role, *b, to(d)))
            arrived_everywhere(s, t + h, *b, then)
            if h <= minor:
                b2 = block(d * h)
                add_wait(t + h, lambda b2=b2: k_copy(s, first_role, *b2, me))
                if h < minor:
                    add_send(t + h, lambda b2=b2: k_copy(s, first_role + 1, *b2, to(-d)))
                arrived_everywhere(s, t + h, *b2, then)

    second_a = lambda t, by, bz: along(0, t, by, bz, "y", dir_of(bz), 2, None)
    second_b = lambda t, by, bz: along(1, t, by, bz, "z", dir_of(by), 2, None)
    arrived_everywhere(1, 0, y, z, second_b)
    along(1, 0, y, z, "y", 1, 0, second_b)
    arrived_everywhere(0, 0, y, z, second_a)
    along(0, 0, y, z, "z", 1, 0, second_a)

    for piece in (2, 0, 1):
        add_send(0, lambda piece=piece: w_copy(x, piece, 0, wrap(x + 1, NX)))
        add_send(0, lambda piece=piece: w_copy(x, piece, 1, wrap(x - 1, NX)))
    before, after, far = wrap(x - 1, NX), wrap(x + 1, NX), wrap(x + 2, NX)
    for piece in (2, 0, 1):
        for bx in (before, after):
            add_wait(4, lambda bx=bx, piece=piece: w_copy(bx, piece, 0, x))
            add_send(4, lambda bx=bx, piece=piece: wp_copy(bx, piece, c))
        if piece == 1:
            add_send(4, lambda: w_copy(after, 1, 3, before))
        else:
            add_send(4, lambda piece=piece: w_copy(before, piece, 2, after))
    for piece in (2, 0, 1):
        add_wait(7, lambda piece=piece: w_copy(far, piece, 0, x))
        add_send(7, lambda piece=piece: wp_copy(far, piece, c))

    scale = score_scale
    row_pos = me * pos + lax.bitwise_and(lax.broadcasted_iota(jnp.int32, (rows, 1), 0), pos - 1)
    contract_last = (((1,), (1,)), ((), ()))
    def fold(s, bz):
        run = NC * pos
        k = jnp.concatenate(
            [keys[s, pl.ds(pl.multiple_of(device_at(by, bz, 0) * pos, run), run), :] for by in range(NY)], axis=0
        )
        count = NY * run
        sc = lax.dot_general(qrows[s], k, contract_last, preferred_element_type=jnp.float32) * scale
        lane = lax.broadcasted_iota(jnp.int32, (1, count), 1)
        key_pos = lax.shift_right_logical(lane, 7) * (NZ * run) + bz * run + lax.bitwise_and(lane, run - 1)
        limit = jnp.minimum(row_pos + 1, len_ref[s])
        sc = jnp.where(key_pos < limit, sc, -jnp.inf)
        old = top[s]
        new = jnp.maximum(old, jnp.max(sc, axis=1, keepdims=True))
        factor = jnp.exp(old - new)
        p = jnp.exp(sc - new[:, 0:1])
        top[s] = new
        total[s] = total[s] * factor + jnp.sum(p, axis=1, keepdims=True)
        acc[s] = acc[s] * factor[:, 0:1] + bdot(p.astype(jnp.bfloat16), k)

    pl.semaphore_wait(barrier, len(expert_ids) + 2)
    for load in loads:
        load.wait()
    for act in rounds[0]:
        act()

    for s in range(2):
        for h in range(HEADS):
            qrows[s, h * pos : (h + 1) * pos, :] = q_ref[:, s, h * lat : (h + 1) * lat]
    for s in range(2):
        k = mem_ref[:, s, :]
        sc = lax.dot_general(qrows[s], k, contract_last, preferred_element_type=jnp.float32) * scale
        m = jnp.max(sc, axis=1, keepdims=True)
        p = jnp.exp(sc - m)
        top[s] = jnp.broadcast_to(m, (rows, 128))
        total[s] = jnp.broadcast_to(jnp.sum(p, axis=1, keepdims=True), (rows, 128))
        acc[s] = bdot(p.astype(jnp.bfloat16), k)

    def round_step(t, carry):
        for r in range(1, 7):

            @pl.when(t == r)
            def _():
                for act in rounds[r]:
                    act()

        u = t - 2

        @pl.when(u >= 0)
        def _():
            count = jnp.where((u == 0) | (u == 4), 1, 2)

            def piece(v, carry2):
                bz = wrap(z + u * (1 - 2 * v), NZ)
                for by in range(NY):
                    for s in range(2):
                        p_copy(s, by, bz, 1 - c).wait_recv()
                for s in range(2):
                    fold(s, bz)
                return carry2

            lax.fori_loop(0, count, piece, 0)

        return carry

    lax.fori_loop(1, 7, round_step, 0)
    for act in rounds[7]:
        act()

    for bx in (before, after, far):
        for piece in range(3):
            wp_copy(bx, piece, 1 - c).wait_recv()

    heads = []
    per = wuv.shape[1]
    for h in range(HEADS):
        part = []
        for s in range(2):
            one = slice(h * pos, (h + 1) * pos)
            part.append((acc[s, one, :] * (1.0 / total[s, one, 0:1])).astype(jnp.bfloat16))
        mixed = jnp.concatenate(part, axis=0)
        heads.append(bdot(mixed, wuv[h // per, h % per]).astype(jnp.bfloat16))
    values = jnp.concatenate(heads, axis=1)
    width = nq_ref.shape[2]
    squares = jnp.zeros((TOK, 1), jnp.float32)
    deep = wout.shape[0] * wout.shape[1]
    for j in range(Q):
        cols = slice(j * width, (j + 1) * width)
        res = bdot(values, wout[:, :, cols].reshape(deep, width)) + jnp.concatenate([hid_ref[:, s, cols] for s in range(2)], axis=0).astype(jnp.float32)
        resid_ref[:, cols] = res
        squares = squares + jnp.sum(res * res, axis=1, keepdims=True)
    rs = lax.rsqrt(squares / (Q * width) + norm_eps)
    for j in range(Q):
        cols = slice(j * width, (j + 1) * width)
        nq_ref[j] = (resid_ref[:, cols] * rs * gain_ref[:, cols].astype(jnp.float32)).astype(jnp.bfloat16)

    for make in sends:
        make().wait_send()


def run_attention(lat, q, mem, lengths, hid, gain, w_uv, w_out):
    anywhere = pl.BlockSpec(memory_space=pl.ANY)
    vmem = pl.BlockSpec(memory_space=pltpu.VMEM)
    bf16, f32 = jnp.bfloat16, jnp.float32
    dma = pltpu.SemaphoreType.DMA
    pos, seqs, lat_dim = lat.shape
    rows = HEADS * pos
    model_width = hid.shape[2]
    blocks = NY * NZ
    return pl.pallas_call(
        attend_kernel,
        out_shape=(
            jax.ShapeDtypeStruct((Q, TOK, model_width // Q), bf16),
            jax.ShapeDtypeStruct((TOK, model_width), f32),
        ),
        in_specs=[vmem, vmem, vmem, pl.BlockSpec(memory_space=pltpu.SMEM), vmem, vmem, anywhere, anywhere],
        out_specs=(vmem, vmem),
        scratch_shapes=[
            pltpu.VMEM((seqs, SEGKEYS * pos, lat_dim), bf16),
            pltpu.VMEM((seqs, rows, lat_dim), bf16),
            pltpu.VMEM((seqs, rows, lat_dim), f32),
            pltpu.VMEM((seqs, rows, 128), f32),
            pltpu.VMEM((seqs, rows, 128), f32),
            pltpu.VMEM((NX,) + w_uv.shape, bf16),
            pltpu.VMEM((NX,) + w_out.shape, bf16),
            dma((4,)),
            dma((seqs, 4, blocks)), dma((seqs, blocks)), dma((seqs, blocks)), dma((seqs, blocks)),
            dma((4, 3)), dma((NX, 3)), dma((NX, 3)), dma((NX, 3)),
        ],
        compiler_params=pltpu.CompilerParams(
            collective_id=0, has_side_effects=True, vmem_limit_bytes=60 * 1024 * 1024
        ),
        name="attend",
    )(lat, q, mem, lengths, hid, gain, w_uv, w_out)


def shards(
    hidden,
    queries,
    latents,
    mem_latents,
    lengths,
    ids,
    gates,
    norm_gain,
    w_uv,
    w_out,
    w_gate,
    w_up,
    w_down,
):
    _, local_len, seq_count, model_width = hidden.shape
    lat = latents[0]
    q = queries[0]
    mem = mem_latents[0]
    hid = hidden[0]
    ids_t = ids[0].transpose(2, 1, 0).reshape(-1, TOK)
    gates_t = gates[0].transpose(2, 1, 0).reshape(-1, TOK)
    nq, resid = run_attention(lat, q, mem, lengths[0], hid, norm_gain[None], w_uv, w_out)
    out = run_experts(
        nq, resid, ids_t, gates_t, jnp.swapaxes(w_gate[0], 0, 1), jnp.swapaxes(w_up[0], 0, 1), w_down[0]
    )
    return out[None]


def solution(mesh):
    return jax.shard_map(
        shards,
        mesh=mesh,
        in_specs=(
            P("dp", "expert", None, None),
            P("dp", "expert", None, None),
            P("dp", "expert", None, None),
            P("dp", None, None, None),
            P("dp", None),
            P("dp", "expert", None, None),
            P("dp", "expert", None, None),
            P(),
            P("dp", None, None),
            P("dp", None),
            P("expert", None, None),
            P("expert", None, None),
            P("expert", None, None),
        ),
        out_specs=P("dp", "expert", None, None),
        check_vma=False,
    )
```

```python
import jax
import jax.numpy as jnp
from jax import lax
from jax.experimental import pallas as pl
from jax.experimental.pallas import tpu as pltpu
from jax.sharding import PartitionSpec as P

score_scale = 192.0 ** (-0.5)
norm_eps = 1e-06


NY, NZ, NC = 4, 8, 2
Q = 8
ADVANCE = 1
HOP1, NEAR_AT, HOP2, HOP3 = 1, 2, 2, 3
FAR_AT = HOP3 + 1
FFN_NEAR = NEAR_AT + 3
FFN_FAR = FAR_AT + 2
RET_NEAR = 2
MIX_FAR, MIX_NEAR = 2, RET_NEAR + 2
SUM1 = MIX_FAR + 1
SUM2 = MIX_NEAR
SUM3 = SUM2 + 1
LAST = SUM3 + 1
TOK = 128
CAP = 14
EXPERTS = 64
PEERS = NY * NC
ROWS = NZ * CAP
ALLROWS = PEERS * ROWS
NEAR = 4
REL = (0, -1, 1, -2, 2, -3, 3, 4)
SLOT = {r: i for i, r in enumerate(REL)}
GROUPS = NZ // NEAR
GROWS = NEAR * CAP
HALF = PEERS * GROWS


def place():
    me = lax.axis_index("expert")
    c = lax.rem(me, NC)
    z = lax.rem(lax.div(me, NC), NZ)
    y = lax.div(me, NC * NZ)
    return me, y, z, c


def device_at(y, z, c):
    return (y * NZ + z) * NC + c


def wrap(v, n):
    return lax.rem(v + 2 * n, n)


def send(src, dst, ssem, rsem, to):
    return pltpu.make_async_remote_copy(
        src_ref=src,
        dst_ref=dst,
        send_sem=ssem,
        recv_sem=rsem,
        device_id={"expert": to},
        device_id_type=pl.DeviceIdType.MESH,
    )


def bdot(a, b):
    return jnp.dot(a, b, preferred_element_type=jnp.float32)


def expert_kernel(
    nq_hbm, resid_hbm, ids_ref, gates_ref, wg_hbm, wu_hbm, wd_hbm, out_ref,
    xs, place_m, mix_m, sent, got, gate_acc, up_acc, act, wg, wu, wd, back, part, landed, resid, table,
    load_sem, zsend, zrecv, ysend, yrecv, osend, orecv, rsend, rrecv, tsend, trecv,
):
    width = xs.shape[3]
    me, y, z, c = place()
    my_slot = y * NC + c
    right = device_at(y, wrap(z + 1, NZ), c)
    left = device_at(y, wrap(z - 1, NZ), c)

    loads = [
        pltpu.make_async_copy(nq_hbm, xs.at[0], load_sem.at[0]),
        pltpu.make_async_copy(wg_hbm, wg, load_sem.at[1]),
        pltpu.make_async_copy(wu_hbm, wu, load_sem.at[2]),
        pltpu.make_async_copy(wd_hbm, wd, load_sem.at[3]),
        pltpu.make_async_copy(resid_hbm, resid, load_sem.at[4]),
    ]
    for load in loads:
        load.start()

    barrier = pltpu.get_barrier_semaphore()

    def peer(k):
        slot = wrap(my_slot + k, PEERS)
        return slot, device_at(lax.div(slot, NC), z, lax.rem(slot, NC))

    partners = [peer(k)[1] for k in range(1, PEERS)] + [right, left]
    for dev in partners:
        pl.semaphore_signal(barrier, inc=1, device_id={"expert": dev}, device_id_type=pl.DeviceIdType.MESH)

    expert_iota = lax.broadcasted_iota(jnp.int32, (EXPERTS, TOK), 0)
    hits = []
    named = jnp.zeros((EXPERTS, TOK), jnp.float32)
    for k in range(6):
        row = jnp.concatenate([ids_ref[k, 0:1, :], ids_ref[k, 1:2, :]], axis=1)
        hit = expert_iota == jnp.broadcast_to(row, (EXPERTS, TOK))
        hits.append(hit)
        named = named + jnp.where(hit, 1.0, 0.0)
    earlier = lax.broadcasted_iota(jnp.int32, (TOK, TOK), 0) < lax.broadcasted_iota(jnp.int32, (TOK, TOK), 1)
    before = bdot(named.astype(jnp.bfloat16), jnp.where(earlier, 1.0, 0.0).astype(jnp.bfloat16))
    expert_base = (expert_iota * CAP).astype(jnp.float32)
    rows = []
    for k in range(6):
        rows.append(jnp.sum(jnp.where(hits[k], before + expert_base, 0.0), axis=0, keepdims=True))
    filler = jnp.full((2, TOK), -1.0, jnp.float32)
    gate_rows = []
    for k in range(6):
        both = gates_ref[k].astype(jnp.float32)
        gate_rows.append(jnp.concatenate([both[0:1], both[1:2]], axis=1))
    table[0] = jnp.concatenate(rows + [filler] + gate_rows + [filler], axis=0)

    gate_acc[...] = jnp.zeros_like(gate_acc)
    up_acc[...] = jnp.zeros_like(up_acc)

    pl.semaphore_wait(barrier, len(partners))
    loads[0].wait()

    def z_hop(j, h, sign):
        src = SLOT[-sign * h]
        dst = SLOT[-sign * (h + 1)] if h < 3 else SLOT[4]
        sem = 6 if h == 3 else h + (0 if sign > 0 else 3)
        return send(xs.at[src, j], xs.at[dst, j], zsend.at[j, sem], zrecv.at[j, dst], right if sign > 0 else left)

    def t_hop(h, sign):
        src = SLOT[-sign * h]
        dst = SLOT[-sign * (h + 1)] if h < 3 else SLOT[4]
        sem = 6 if h == 3 else h + (0 if sign > 0 else 3)
        return send(table.at[src], table.at[dst], tsend.at[sem], trecv.at[dst], right if sign > 0 else left)

    def z_here(j, slot):
        send(xs.at[slot, j], xs.at[slot, j], zsend.at[j, 0], zrecv.at[j, slot], right).wait_recv()

    def t_here(slot):
        send(table.at[slot], table.at[slot], tsend.at[0], trecv.at[slot], right).wait_recv()

    def y_copy(k, j, g):
        slot, to = peer(k)
        return send(sent.at[j, g, slot], got.at[j, g, my_slot], ysend.at[g, j, k], yrecv.at[g, j, my_slot], to)

    def y_here(k, j, g):
        slot, to = peer(k)
        send(sent.at[j, g, slot], got.at[j, g, slot], ysend.at[g, j, k], yrecv.at[g, j, slot], to).wait_recv()

    def o_copy(k, j, g):
        slot, to = peer(k)
        return send(sent.at[j, g, slot], back.at[j, g, my_slot], osend.at[g, j, k], orecv.at[g, j, my_slot], to)

    def o_here(k, j, g):
        slot, to = peer(k)
        send(sent.at[j, g, slot], back.at[j, g, slot], osend.at[g, j, k], orecv.at[g, j, slot], to).wait_recv()

    def parity(j):
        return lax.rem(z + j, 2)

    def build_tables(g):
        r = lax.broadcasted_iota(jnp.int32, (HALF, TOK), 0)
        group = lax.shift_right_logical(r * 9363, 17)
        within = r - group * CAP
        owner_slot = lax.shift_right_logical(group, 2)
        near = group - owner_slot * NEAR
        owner_y = lax.shift_right_logical(owner_slot, 1)
        owner_c = owner_slot - owner_y * NC
        owner = (owner_y * NZ + z) * NC + owner_c
        base = owner * CAP + within

        def one_block(b, carry):
            code = jnp.where(near == b, base, -7).astype(jnp.float32)
            rows_b = table[g * NEAR + b]
            hot = jnp.zeros((HALF, TOK), jnp.float32)
            mixed = jnp.zeros((HALF, TOK), jnp.float32)
            for k in range(6):
                hit = code == jnp.broadcast_to(rows_b[k : k + 1, :], (HALF, TOK))
                hot = jnp.where(hit, 1.0, hot)
                mixed = jnp.where(hit, jnp.broadcast_to(rows_b[8 + k : 9 + k, :], (HALF, TOK)), mixed)
            place_m[g, :, pl.ds(pl.multiple_of(b * TOK, TOK), TOK)] = hot.astype(jnp.bfloat16)
            mix_m[g, pl.ds(pl.multiple_of(b * TOK, TOK), TOK), :] = mixed.T.astype(jnp.bfloat16)
            return carry

        lax.fori_loop(0, NEAR, one_block, 0)

    def on(cond, f):
        pl.when(cond)(f)

    def valid(j):
        return (j >= 0) & (j < Q)

    def dispatch_step(i, carry):
        def own(j):
            z_hop(j, 0, 1).start()
            z_hop(j, 0, -1).start()

        @pl.when(i == 0)
        def _():
            t_hop(0, 1).start()
            t_hop(0, -1).start()
            for j in range(ADVANCE):
                own(j)

        on(i + ADVANCE < Q, lambda: own(i + ADVANCE))

        def forward(j, h, hop, here):
            here(j, SLOT[-h])
            if h < 3:
                hop(j, h, 1).start()
            here(j, SLOT[h])
            if h < 3:
                hop(j, h, -1).start()
            else:
                on(parity(j) == 1, lambda: hop(j, 3, 1).start())
                on(parity(j) == 0, lambda: hop(j, 3, -1).start())

        def compact(j, g):
            block_rows = xs[g * NEAR : (g + 1) * NEAR, j].reshape(NEAR * TOK, width)
            packed = bdot(place_m[g], block_rows).astype(jnp.bfloat16)
            sent[j, g] = packed.reshape(PEERS, GROWS, width)
            got[j, g, my_slot] = sent[j, g, my_slot]

        def ship(j, g):
            for k in range(1, PEERS):
                y_copy(k, j, g).start()

        def feed(j, g):
            for k in range(1, PEERS):
                y_here(k, j, g)
            x = got[j, g].reshape(HALF, width)
            cols = pl.ds(pl.multiple_of(j * width, width), width)
            last = (((1,), (1,)), ((), ()))
            gate_acc[g] += lax.dot_general(x, wg[:, cols], last, preferred_element_type=jnp.float32)
            up_acc[g] += lax.dot_general(x, wu[:, cols], last, preferred_element_type=jnp.float32)

        @pl.when(valid(i - HOP1))
        def _():
            forward(i - HOP1, 1, z_hop, z_here)

        for h in (1, 2, 3):
            on(i == h, lambda: forward(0, h, lambda j, k, sign: t_hop(k, sign), lambda j, slot: t_here(slot)))

        jn, j2, j3, jf = i - NEAR_AT, i - HOP2, i - HOP3, i - FAR_AT

        @pl.when(valid(jn))
        def _():
            z_here(jn, SLOT[-2])

        @pl.when(valid(j2))
        def _():
            z_hop(j2, 2, 1).start()
            z_here(j2, SLOT[2])
            z_hop(j2, 2, -1).start()

        on(valid(j3), lambda: forward(j3, 3, z_hop, z_here))
        on(i == 2, lambda: build_tables(0))

        @pl.when(i == 4)
        def _():
            t_here(SLOT[4])
            build_tables(1)

        on(valid(jn), lambda: compact(jn, 0))

        @pl.when(valid(jf))
        def _():
            z_here(jf, SLOT[4])
            compact(jf, 1)

        on(valid(jn), lambda: ship(jn, 0))

        @pl.when(i == FFN_NEAR)
        def _():
            loads[1].wait()
            loads[2].wait()

        on(valid(jf), lambda: ship(jf, 1))
        on(valid(i - FFN_NEAR), lambda: feed(i - FFN_NEAR, 0))
        on(valid(i - FFN_FAR), lambda: feed(i - FFN_FAR, 1))
        return carry

    lax.fori_loop(0, Q + FFN_FAR, dispatch_step, 0)

    g = gate_acc[...]
    act[...] = ((g / (1.0 + jnp.exp(-g))) * up_acc[...]).astype(jnp.bfloat16)
    loads[3].wait()
    loads[4].wait()

    def drain_dispatch(j, carry):
        for h in range(3):
            z_hop(j, h, 1).wait_send()
            z_hop(j, h, -1).wait_send()
        z_hop(j, 3, 1).wait_send()
        for g in range(GROUPS):
            for k in range(1, PEERS):
                y_copy(k, j, g).wait_send()
        return carry

    lax.fori_loop(0, Q, drain_dispatch, 0)
    for h in range(3):
        t_hop(h, 1).wait_send()
        t_hop(h, -1).wait_send()
    t_hop(3, 1).wait_send()

    def r_copy(j, k, to):
        return send(xs.at[k, j], landed.at[k, j], rsend.at[j, k], rrecv.at[j, k], to)

    def r_here(j, k):
        r_copy(j, k, right).wait_recv()

    def wide(j, k):
        return landed[k, j].astype(jnp.float32)

    def combine_step(i, carry):
        def make(j, g):
            cols = pl.ds(pl.multiple_of(j * width, width), width)
            made = bdot(act[g], wd[:, cols]).astype(jnp.bfloat16)
            sent[j, g] = made.reshape(PEERS, GROWS, width)
            back[j, g, my_slot] = sent[j, g, my_slot]

        def mix(j, g):
            for k in range(1, PEERS):
                o_here(k, j, g)
            mixed = bdot(mix_m[g], back[j, g].reshape(HALF, width))
            part[j, g * NEAR : (g + 1) * NEAR] = mixed.reshape(NEAR, TOK, width)

        def ship_back(j, g):
            for k in range(1, PEERS):
                o_copy(k, j, g).start()

        on(i < Q, lambda: make(i, 1))
        on(valid(i - RET_NEAR), lambda: make(i - RET_NEAR, 0))
        j0, j1, j2, j3, j4 = i - MIX_FAR, i - SUM1, i - SUM2, i - SUM3, i - LAST

        @pl.when(valid(j0))
        def _():
            mix(j0, 1)
            xs[0, j0] = part[j0, SLOT[4]].astype(jnp.bfloat16)

        @pl.when(valid(j1))
        def _():
            r_here(j1, 0)
            odd = (parity(j1) == 1).astype(jnp.float32)
            arrived = wide(j1, 0)
            xs[1, j1] = (part[j1, SLOT[3]] + arrived * odd).astype(jnp.bfloat16)
            xs[4, j1] = (part[j1, SLOT[-3]] + arrived * (1.0 - odd)).astype(jnp.bfloat16)

        on(i < Q, lambda: ship_back(i, 1))
        on(valid(i - RET_NEAR), lambda: ship_back(i - RET_NEAR, 0))

        @pl.when(valid(j0))
        def _():
            on(parity(j0) == 0, lambda: r_copy(j0, 0, right).start())
            on(parity(j0) == 1, lambda: r_copy(j0, 0, left).start())

        on(valid(i - MIX_NEAR), lambda: mix(i - MIX_NEAR, 0))

        def add_on(j, s):
            r_here(j, s - 1)
            xs[s, j] = (part[j, SLOT[4 - s]] + wide(j, s - 1)).astype(jnp.bfloat16)
            r_here(j, s + 2)
            xs[s + 3, j] = (part[j, SLOT[s - 4]] + wide(j, s + 2)).astype(jnp.bfloat16)

        def pass_on(j, s):
            r_copy(j, s, right).start()
            r_copy(j, s + 3, left).start()

        on(valid(j1), lambda: pass_on(j1, 1))
        on(valid(j3), lambda: add_on(j3, 3))
        on(valid(j2), lambda: add_on(j2, 2))
        on(valid(j3), lambda: pass_on(j3, 3))
        on(valid(j2), lambda: pass_on(j2, 2))

        @pl.when(valid(j4))
        def _():
            r_here(j4, 3)
            r_here(j4, 6)
            total = part[j4, 0] + wide(j4, 3) + wide(j4, 6)
            cols = pl.ds(pl.multiple_of(j4 * width, width), width)
            final = (resid[:, cols] + total).astype(jnp.bfloat16)
            for s in range(2):
                out_ref[:, s, cols] = final[s * (TOK // 2) : (s + 1) * (TOK // 2)]

        return carry

    lax.fori_loop(0, Q + LAST, combine_step, 0)

    def drain_combine(j, carry):
        for k in range(7):
            r_copy(j, k, right).wait_send()
        for g in range(GROUPS):
            for k in range(1, PEERS):
                o_copy(k, j, g).wait_send()
        return carry

    lax.fori_loop(0, Q, drain_combine, 0)


def run_experts(nq, resid, ids_t, gates_t, w_gate, w_up, w_down):
    width = nq.shape[2]
    hidden_units, model_width = w_gate.shape
    anywhere = pl.BlockSpec(memory_space=pl.ANY)
    vmem = pl.BlockSpec(memory_space=pltpu.VMEM)
    bf16, f32 = jnp.bfloat16, jnp.float32
    dma = pltpu.SemaphoreType.DMA
    return pl.pallas_call(
        expert_kernel,
        out_shape=jax.ShapeDtypeStruct((TOK // 2, 2, model_width), bf16),
        in_specs=[anywhere, anywhere, vmem, vmem, anywhere, anywhere, anywhere],
        out_specs=vmem,
        scratch_shapes=[
            pltpu.VMEM((NZ, Q, TOK, width), bf16),
            pltpu.VMEM((GROUPS, HALF, NEAR * TOK), bf16),
            pltpu.VMEM((GROUPS, NEAR * TOK, HALF), bf16),
            pltpu.VMEM((Q, GROUPS, PEERS, GROWS, width), bf16),
            pltpu.VMEM((Q, GROUPS, PEERS, GROWS, width), bf16),
            pltpu.VMEM((GROUPS, HALF, hidden_units), f32),
            pltpu.VMEM((GROUPS, HALF, hidden_units), f32),
            pltpu.VMEM((GROUPS, HALF, hidden_units), bf16),
            pltpu.VMEM((hidden_units, model_width), bf16),
            pltpu.VMEM((hidden_units, model_width), bf16),
            pltpu.VMEM((hidden_units, model_width), bf16),
            pltpu.VMEM((Q, GROUPS, PEERS, GROWS, width), bf16),
            pltpu.VMEM((Q, NZ, TOK, width), f32),
            pltpu.VMEM((7, Q, TOK, width), bf16),
            pltpu.VMEM((TOK, model_width), f32),
            pltpu.VMEM((NZ, 16, TOK), f32),
            dma((5,)),
            dma((Q, 7)), dma((Q, NZ)), dma((GROUPS, Q, PEERS)), dma((GROUPS, Q, PEERS)), dma((GROUPS, Q, PEERS)), dma((GROUPS, Q, PEERS)),
            dma((Q, 7)), dma((Q, 7)), dma((7,)), dma((NZ,)),
        ],
        compiler_params=pltpu.CompilerParams(
            collective_id=1, has_side_effects=True, vmem_limit_bytes=60 * 1024 * 1024
        ),
        name="experts",
    )(nq, resid, ids_t, gates_t, w_gate, w_up, w_down)


HEADS = 8
NX = 4
SEGKEYS = NY * NZ * NC


def attend_kernel(
    lat_hbm, q_ref, mem_ref, len_ref, hid_ref, gain_ref, wuv_hbm, wout_hbm, nq_ref, resid_ref,
    keys, qrows, acc, top, total, wuv, wout,
    load_sem, ksend, krecv, psend, precv, wsend, wrecv, wpsend, wprecv,
):
    me, y, z, c = place()
    x = lax.axis_index("dp")
    pos = lat_hbm.shape[0]
    lat = lat_hbm.shape[2]
    rows = HEADS * pos
    partner = device_at(y, z, 1 - c)
    own_start = pl.multiple_of(me * pos, pos)

    loads = [
        pltpu.make_async_copy(wout_hbm, wout.at[x], load_sem.at[2]),
        pltpu.make_async_copy(wuv_hbm, wuv.at[x], load_sem.at[3]),
    ]
    for load in loads:
        load.start()
    for s in range(2):
        keys[s, pl.ds(own_start, pos), :] = lat_hbm[:, s, :]

    barrier = pltpu.get_barrier_semaphore()
    mesh_id = pl.DeviceIdType.MESH
    expert_ids = [
        device_at(y, wrap(z + 1, NZ), c), device_at(y, wrap(z - 1, NZ), c),
        device_at(wrap(y + 1, NY), z, c), device_at(wrap(y - 1, NY), z, c), partner,
    ]
    for dev in expert_ids:
        pl.semaphore_signal(barrier, inc=1, device_id={"expert": dev}, device_id_type=mesh_id)
    for dev in (wrap(x + 1, NX), wrap(x - 1, NX)):
        pl.semaphore_signal(barrier, inc=1, device_id={"dp": dev}, device_id_type=mesh_id)

    def key_block(s, by, bz, bc):
        return keys.at[s, pl.ds(pl.multiple_of(device_at(by, bz, bc) * pos, pos), pos)]

    def k_copy(s, role, by, bz, to):
        ref = key_block(s, by, bz, c)
        block = by * NZ + bz
        return send(ref, ref, ksend.at[s, role, block], krecv.at[s, block], to)

    def p_copy(s, by, bz, bc):
        ref = key_block(s, by, bz, bc)
        block = by * NZ + bz
        return send(ref, ref, psend.at[s, block], precv.at[s, block], partner)

    def w_pieces(bx, bc):
        half = wout.shape[1] // 2
        sub = half // 2
        first = wout.at[bx, pl.ds(pl.multiple_of(bc * half, half), sub)]
        second = wout.at[bx, pl.ds(pl.multiple_of(bc * half + sub, sub), sub)]
        return [first, second, wuv.at[bx, bc]]

    def w_copy(bx, piece, role, to):
        ref = w_pieces(bx, c)[piece]
        return pltpu.make_async_remote_copy(
            src_ref=ref, dst_ref=ref, send_sem=wsend.at[role, piece], recv_sem=wrecv.at[bx, piece],
            device_id={"dp": to}, device_id_type=mesh_id,
        )

    def wp_copy(bx, piece, bc):
        ref = w_pieces(bx, bc)[piece]
        return send(ref, ref, wpsend.at[bx, piece], wprecv.at[bx, piece], partner)

    rounds = [[] for _ in range(8)]
    sends = []

    def add_send(t, make):
        sends.append(make)
        rounds[t].append(lambda: make().start())

    def add_wait(t, make):
        rounds[t].append(lambda: make().wait_recv())

    def dir_of(v):
        return 1 - 2 * lax.rem(v, 2)

    def arrived_everywhere(s, t, by, bz, second):
        add_send(t, lambda: p_copy(s, by, bz, c))
        if second is not None:
            second(t, by, bz)

    def along(s, t, by, bz, axis, d, first_role, then):
        n = NZ if axis == "z" else NY
        major, minor = n // 2, n - 1 - n // 2

        def to(k):
            return device_at(y, wrap(z + k, NZ), c) if axis == "z" else device_at(wrap(y + k, NY), z, c)

        def block(k):
            return (by, wrap(bz + k, NZ)) if axis == "z" else (wrap(by + k, NY), bz)

        add_send(t, lambda: k_copy(s, first_role, by, bz, to(d)))
        add_send(t, lambda: k_copy(s, first_role + 1, by, bz, to(-d)))
        for h in range(1, major + 1):
            b = block(-d * h)
            add_wait(t + h, lambda b=b: k_copy(s, first_role, *b, me))
            if h < major:
                add_send(t + h, lambda b=b: k_copy(s, first_role, *b, to(d)))
            arrived_everywhere(s, t + h, *b, then)
            if h <= minor:
                b2 = block(d * h)
                add_wait(t + h, lambda b2=b2: k_copy(s, first_role, *b2, me))
                if h < minor:
                    add_send(t + h, lambda b2=b2: k_copy(s, first_role + 1, *b2, to(-d)))
                arrived_everywhere(s, t + h, *b2, then)

    second_a = lambda t, by, bz: along(0, t, by, bz, "y", dir_of(bz), 2, None)
    second_b = lambda t, by, bz: along(1, t, by, bz, "z", dir_of(by), 2, None)
    arrived_everywhere(1, 0, y, z, second_b)
    along(1, 0, y, z, "y", 1, 0, second_b)
    arrived_everywhere(0, 0, y, z, second_a)
    along(0, 0, y, z, "z", 1, 0, second_a)

    for piece in (2, 0, 1):
        add_send(0, lambda piece=piece: w_copy(x, piece, 0, wrap(x + 1, NX)))
        add_send(0, lambda piece=piece: w_copy(x, piece, 1, wrap(x - 1, NX)))
    before, after, far = wrap(x - 1, NX), wrap(x + 1, NX), wrap(x + 2, NX)
    for piece in (2, 0, 1):
        for bx in (before, after):
            add_wait(4, lambda bx=bx, piece=piece: w_copy(bx, piece, 0, x))
            add_send(4, lambda bx=bx, piece=piece: wp_copy(bx, piece, c))
        if piece == 1:
            add_send(4, lambda: w_copy(after, 1, 3, before))
        else:
            add_send(4, lambda piece=piece: w_copy(before, piece, 2, after))
    for piece in (2, 0, 1):
        add_wait(7, lambda piece=piece: w_copy(far, piece, 0, x))
        add_send(7, lambda piece=piece: wp_copy(far, piece, c))

    scale = score_scale
    row_pos = me * pos + lax.bitwise_and(lax.broadcasted_iota(jnp.int32, (rows, 1), 0), pos - 1)
    contract_last = (((1,), (1,)), ((), ()))
    def fold(s, bz):
        run = NC * pos
        k = jnp.concatenate(
            [keys[s, pl.ds(pl.multiple_of(device_at(by, bz, 0) * pos, run), run), :] for by in range(NY)], axis=0
        )
        count = NY * run
        sc = lax.dot_general(qrows[s], k, contract_last, preferred_element_type=jnp.float32) * scale
        lane = lax.broadcasted_iota(jnp.int32, (1, count), 1)
        key_pos = lax.shift_right_logical(lane, 7) * (NZ * run) + bz * run + lax.bitwise_and(lane, run - 1)
        limit = jnp.minimum(row_pos + 1, len_ref[s])
        sc = jnp.where(key_pos < limit, sc, -jnp.inf)
        old = top[s]
        new = jnp.maximum(old, jnp.max(sc, axis=1, keepdims=True))
        factor = jnp.exp(old - new)
        p = jnp.exp(sc - new[:, 0:1])
        top[s] = new
        total[s] = total[s] * factor + jnp.sum(p, axis=1, keepdims=True)
        acc[s] = acc[s] * factor[:, 0:1] + bdot(p.astype(jnp.bfloat16), k)

    pl.semaphore_wait(barrier, len(expert_ids) + 2)
    for load in loads:
        load.wait()
    for act in rounds[0]:
        act()

    for s in range(2):
        for h in range(HEADS):
            qrows[s, h * pos : (h + 1) * pos, :] = q_ref[:, s, h * lat : (h + 1) * lat]
    for s in range(2):
        k = mem_ref[:, s, :]
        sc = lax.dot_general(qrows[s], k, contract_last, preferred_element_type=jnp.float32) * scale
        m = jnp.max(sc, axis=1, keepdims=True)
        p = jnp.exp(sc - m)
        top[s] = jnp.broadcast_to(m, (rows, 128))
        total[s] = jnp.broadcast_to(jnp.sum(p, axis=1, keepdims=True), (rows, 128))
        acc[s] = bdot(p.astype(jnp.bfloat16), k)

    def round_step(t, carry):
        for r in range(1, 7):

            @pl.when(t == r)
            def _():
                for act in rounds[r]:
                    act()

        u = t - 2

        @pl.when(u >= 0)
        def _():
            count = jnp.where((u == 0) | (u == 4), 1, 2)

            def piece(v, carry2):
                bz = wrap(z + u * (1 - 2 * v), NZ)
                for by in range(NY):
                    for s in range(2):
                        p_copy(s, by, bz, 1 - c).wait_recv()
                for s in range(2):
                    fold(s, bz)
                return carry2

            lax.fori_loop(0, count, piece, 0)

        return carry

    lax.fori_loop(1, 7, round_step, 0)
    for act in rounds[7]:
        act()

    for bx in (before, after, far):
        for piece in range(3):
            wp_copy(bx, piece, 1 - c).wait_recv()

    heads = []
    per = wuv.shape[1]
    for h in range(HEADS):
        part = []
        for s in range(2):
            one = slice(h * pos, (h + 1) * pos)
            part.append((acc[s, one, :] * (1.0 / total[s, one, 0:1])).astype(jnp.bfloat16))
        mixed = jnp.concatenate(part, axis=0)
        heads.append(bdot(mixed, wuv[h // per, h % per]).astype(jnp.bfloat16))
    values = jnp.concatenate(heads, axis=1)
    width = nq_ref.shape[2]
    squares = jnp.zeros((TOK, 1), jnp.float32)
    deep = wout.shape[0] * wout.shape[1]
    for j in range(Q):
        cols = slice(j * width, (j + 1) * width)
        res = bdot(values, wout[:, :, cols].reshape(deep, width)) + jnp.concatenate([hid_ref[:, s, cols] for s in range(2)], axis=0).astype(jnp.float32)
        resid_ref[:, cols] = res
        squares = squares + jnp.sum(res * res, axis=1, keepdims=True)
    rs = lax.rsqrt(squares / (Q * width) + norm_eps)
    for j in range(Q):
        cols = slice(j * width, (j + 1) * width)
        nq_ref[j] = (resid_ref[:, cols] * rs * gain_ref[cols].astype(jnp.float32).reshape(1, width)).astype(jnp.bfloat16)

    for make in sends:
        make().wait_send()


def run_attention(lat, q, mem, lengths, hid, gain, w_uv, w_out):
    anywhere = pl.BlockSpec(memory_space=pl.ANY)
    vmem = pl.BlockSpec(memory_space=pltpu.VMEM)
    bf16, f32 = jnp.bfloat16, jnp.float32
    dma = pltpu.SemaphoreType.DMA
    pos, seqs, lat_dim = lat.shape
    rows = HEADS * pos
    model_width = hid.shape[2]
    blocks = NY * NZ
    return pl.pallas_call(
        attend_kernel,
        out_shape=(
            jax.ShapeDtypeStruct((Q, TOK, model_width // Q), bf16),
            jax.ShapeDtypeStruct((TOK, model_width), f32),
        ),
        in_specs=[vmem, vmem, vmem, pl.BlockSpec(memory_space=pltpu.SMEM), vmem, vmem, anywhere, anywhere],
        out_specs=(vmem, vmem),
        scratch_shapes=[
            pltpu.VMEM((seqs, SEGKEYS * pos, lat_dim), bf16),
            pltpu.VMEM((seqs, rows, lat_dim), bf16),
            pltpu.VMEM((seqs, rows, lat_dim), f32),
            pltpu.VMEM((seqs, rows, 128), f32),
            pltpu.VMEM((seqs, rows, 128), f32),
            pltpu.VMEM((NX,) + w_uv.shape, bf16),
            pltpu.VMEM((NX,) + w_out.shape, bf16),
            dma((4,)),
            dma((seqs, 4, blocks)), dma((seqs, blocks)), dma((seqs, blocks)), dma((seqs, blocks)),
            dma((4, 3)), dma((NX, 3)), dma((NX, 3)), dma((NX, 3)),
        ],
        compiler_params=pltpu.CompilerParams(
            collective_id=0, has_side_effects=True, vmem_limit_bytes=60 * 1024 * 1024
        ),
        name="attend",
    )(lat, q, mem, lengths, hid, gain, w_uv, w_out)


def shards(
    hidden,
    queries,
    latents,
    mem_latents,
    lengths,
    ids,
    gates,
    norm_gain,
    w_uv,
    w_out,
    w_gate,
    w_up,
    w_down,
):
    _, local_len, seq_count, model_width = hidden.shape
    lat = latents[0]
    q = queries[0]
    mem = mem_latents[0]
    hid = hidden[0]
    ids_t = ids[0].transpose(2, 1, 0)
    gates_t = gates[0].transpose(2, 1, 0)
    nq, resid = run_attention(lat, q, mem, lengths[0], hid, norm_gain, w_uv, w_out)
    out = run_experts(
        nq, resid, ids_t, gates_t, jnp.swapaxes(w_gate[0], 0, 1), jnp.swapaxes(w_up[0], 0, 1), w_down[0]
    )
    return out[None]


def solution(mesh):
    return jax.shard_map(
        shards,
        mesh=mesh,
        in_specs=(
            P("dp", "expert", None, None),
            P("dp", "expert", None, None),
            P("dp", "expert", None, None),
            P("dp", None, None, None),
            P("dp", None),
            P("dp", "expert", None, None),
            P("dp", "expert", None, None),
            P(),
            P("dp", None, None),
            P("dp", None),
            P("expert", None, None),
            P("expert", None, None),
            P("expert", None, None),
        ),
        out_specs=P("dp", "expert", None, None),
        check_vma=False,
    )
```
